32 devices in a mesh: rep: 2 (over x), ctx: 16 (over z, y, core).
Axes of the slice: x: 2, y: 2, z: 4, core: 2. Of those that a mesh axis runs over, the one named last changes fastest.
Arguments:
- queries: bfloat16 [4096, 32, 128], P(('rep', 'ctx')), parts along dimension 0, may hold values from -128 to 128
- keys: bfloat16 [4096, 2, 128], P(('rep', 'ctx')), parts along dimension 0, may hold values from -5 to 5
- values: bfloat16 [4096, 2, 128], P(('rep', 'ctx')), parts along dimension 0, may hold values from -6 to 6
- grad_out: bfloat16 [4096, 32, 128], P(('rep', 'ctx')), parts along dimension 0, may hold values from -6 to 6
- selected: int32 [4096, 2, 8], P(('rep', 'ctx')), parts along dimension 0, may hold values from 0 to 31, as said below
Outputs:
- dquery: bfloat16 [4096, 32, 128], P(('rep', 'ctx')), parts along dimension 0
- key_grad: bfloat16 [4096, 2, 128], P(('rep', 'ctx')), parts along dimension 0
- value_grad: bfloat16 [4096, 2, 128], P(('rep', 'ctx')), parts along dimension 0
The draws below stay inside these ranges and needn't reach their ends.
There are 2 independent parts, one for each index of `rep`. The reference program is written for one: setup_inputs(seed, part) draws one part's arguments, and reference() takes and returns one part's arrays. A program takes and returns all parts, laid end to end along the dimension named above; each array names one. Nothing has to cross between parts.
Inputs may be any that keep to these rules, and one draw needn't show every extreme that they name: The 8 blocks of selected[t, g] are different and include block t // 64 and block 0. Over the 128 tokens of one device of ctx, the blocks named for one group that lie on other devices number exactly 7, at most one of each other device; block 0 is among them for every device but the first.
All inputs are finite; a program needn't handle non-finite values.
Results may differ from the reference program's by a relative error of at most 0.0075.
Values may be sent and summed in bfloat16 or wider, within the bound.
A program may use at most 128 MiB of HBM per device.

```python
import math
import jax
import jax.numpy as jnp
from jax import lax

HEADS = 32
KVG = 2
DH = 128
BLK = 64
SEL = 8
TOK_DEV = 128
BPD = 2
OTHERS = 6
FG = 7
POOLB = 9
SEQ = 2048
N_CTX = 16


def choose_blocks(key):
    base = jax.random.fold_in(key, 11)
    first, second, third, fourth = jax.random.split(base, 4)
    requesters = jnp.arange(N_CTX).astype(jnp.int32)[:, None]
    owner_ids = jnp.arange(N_CTX).astype(jnp.int32)[None, :]
    noise = jax.random.randint(first, (N_CTX, N_CTX), 0, 1 << 20)
    ranking = noise * N_CTX + owner_ids + jnp.where(owner_ids < requesters, 1 << 27, 0)
    ranking = jnp.where((owner_ids == requesters) | (owner_ids == 0), -1, ranking)
    unused, ranked = lax.top_k(ranking, FG)
    with_sink = jnp.concatenate([jnp.zeros((N_CTX, 1), jnp.int32), ranked[:, :OTHERS]], axis=1)
    owner_list = jnp.where(requesters > 0, with_sink, ranked).astype(jnp.int32)
    local_ids = jax.random.randint(second, (N_CTX, FG, KVG), 0, BPD)
    local_ids = jnp.where(owner_list[..., None] == 0, 0, local_ids)
    far_blocks = owner_list[..., None] * BPD + local_ids
    own_blocks = requesters * BPD + jnp.arange(BPD).astype(jnp.int32)[None, :]
    own_blocks = jnp.broadcast_to(own_blocks[:, :, None], (N_CTX, BPD, KVG))
    pool_ids = jnp.concatenate([own_blocks, far_blocks], axis=1).transpose(0, 2, 1)
    pool_tokens = jnp.repeat(pool_ids, TOK_DEV, axis=0)
    token_ids = jnp.arange(SEQ).astype(jnp.int32)
    slot_ids = jnp.arange(POOLB).astype(jnp.int32)
    needed = (pool_tokens == (token_ids // BLK)[:, None, None]) | (pool_tokens == 0)
    needed = needed | (slot_ids[None, None, :] == (token_ids % TOK_DEV % POOLB)[:, None, None])
    shuffle = jax.random.randint(third, (SEQ, KVG, POOLB), 0, 1 << 20)
    marks = shuffle * POOLB + slot_ids + jnp.where(needed, 1 << 26, 0)
    unused_top, picks = lax.top_k(marks, SEL)
    chosen = jnp.take_along_axis(pool_tokens, picks, axis=2)
    reorder = jax.random.randint(fourth, (SEQ, KVG, SEL), 0, 1 << 20) * SEL + jnp.arange(SEL).astype(jnp.int32)
    order = jnp.argsort(reorder, axis=2)
    return jnp.take_along_axis(chosen, order, axis=2).astype(jnp.int32)


def query_key_pair(key):
    base = jax.random.fold_in(key, 23)
    first, second = jax.random.split(base, 2)
    key_base = jnp.clip(jax.random.normal(first, (SEQ, KVG, DH), jnp.float32), -5.0, 5.0)
    key_vals = key_base
    query_vals = jnp.clip(2.0 * jax.random.normal(second, (SEQ, HEADS, DH), jnp.float32), -12.0, 12.0)
    return (query_vals, key_vals)


def draw_queries(key, part):
    query_vals, key_vals = query_key_pair(key)
    return query_vals.astype(jnp.bfloat16)


def draw_keys(key, part):
    query_vals, key_vals = query_key_pair(key)
    return key_vals.astype(jnp.bfloat16)


def draw_selected(key, part):
    return choose_blocks(key)


def block_levels(stream_key, shape, cuts, low, largest):
    level, own = 1.0, jax.random.fold_in(stream_key, 6)
    for position, blocks in cuts:
        draws = jnp.exp(jax.random.uniform(jax.random.fold_in(own, position), (blocks,), jnp.float32, low / len(cuts), largest / len(cuts)))
        level = level * jnp.repeat(draws, shape[position] // blocks).reshape([-1 if axis == position else 1 for axis in range(len(shape))])
    return level


def normal_values(stream_key, dims, deviation, reach, cuts=(), held_as=jnp.bfloat16):
    entries = jax.random.normal(stream_key, dims, jnp.float32) * deviation
    if len(cuts) > 0:
        entries = block_levels(stream_key, dims, cuts, -0.22, 0.18) * entries
    return jnp.clip(entries, min=-reach, max=reach).astype(held_as)


def setup_inputs(seed: int = 0, part: int = 0) -> dict:
    splits = jax.random.split(jax.random.key(seed), 6)
    own_keys = jax.random.split(jax.random.fold_in(splits[5], part), 6)
    return {
        "queries": draw_queries(jax.random.fold_in(jax.random.fold_in(splits[5], part), 71), part),
        "keys": draw_keys(jax.random.fold_in(jax.random.fold_in(splits[5], part), 71), part),
        "values": normal_values(own_keys[2], (SEQ, KVG, DH), 1.0, 6.0, ((0, 16),)),
        "grad_out": normal_values(own_keys[3], (SEQ, HEADS, DH), 1.0, 6.0, ((0, 16),)),
        "selected": draw_selected(jax.random.fold_in(jax.random.fold_in(splits[5], part), 71), part),
    }


def reference(queries, keys, values, grad_out, selected):
    seq_len, head_count, head_dim = queries.shape
    groups = keys.shape[1]
    per_group = head_count // groups
    scaling = 1.0 / math.sqrt(head_dim)
    tile_rows = min(seq_len, 64)
    step_count = seq_len // tile_rows
    keys_by_group = keys.transpose(1, 0, 2)
    values_by_group = values.transpose(1, 0, 2)
    group_ids = jnp.arange(groups).astype(jnp.int32)[None, :, None]
    offsets = jnp.arange(BLK).astype(jnp.int32)

    def visit(carry, inputs):
        key_acc, value_acc = carry
        query_blk, upstream, chosen, first = inputs
        positions = (chosen[..., None] * BLK + offsets).reshape(tile_rows, groups, -1).astype(jnp.int32)
        key_rows = keys_by_group[group_ids, positions].astype(jnp.float32)
        value_rows = values_by_group[group_ids, positions].astype(jnp.float32)
        query_f = query_blk.astype(jnp.float32).reshape(tile_rows, groups, per_group, head_dim)
        upstream_f = upstream.astype(jnp.float32).reshape(tile_rows, groups, per_group, head_dim)
        scores = jnp.einsum('tghd,tgld->tghl', query_f, key_rows) * scaling
        query_pos = first + jnp.arange(tile_rows).astype(jnp.int32)
        allowed = positions <= query_pos[:, None, None]
        scores = jnp.where(allowed[:, :, None, :], scores, -jnp.inf)
        row_peak = lax.optimization_barrier(jnp.max(scores, axis=-1, keepdims=True))
        weights = jnp.exp(scores - row_peak)
        weights = weights / lax.optimization_barrier(jnp.sum(weights, axis=-1, keepdims=True))
        slope_grad = jnp.einsum('tghd,tgld->tghl', upstream_f, value_rows)
        row_inner = lax.optimization_barrier(jnp.sum(weights * slope_grad, axis=-1, keepdims=True))
        dscore = lax.optimization_barrier((weights * (slope_grad - row_inner) * scaling).astype(jnp.bfloat16))
        weights_low = lax.optimization_barrier(weights.astype(jnp.bfloat16))
        dscore_f = dscore.astype(jnp.float32)
        weights_f = weights_low.astype(jnp.float32)
        dquery = jnp.einsum('tghl,tgld->tghd', dscore_f, key_rows).astype(jnp.bfloat16)
        key_part = jnp.einsum('tghl,tghd->tgld', dscore_f, query_f)
        value_part = jnp.einsum('tghl,tghd->tgld', weights_f, upstream_f)
        key_acc = key_acc.at[group_ids, positions].add(key_part)
        value_acc = value_acc.at[group_ids, positions].add(value_part)
        return ((key_acc, value_acc), dquery.reshape(tile_rows, head_count, head_dim))
    inputs = (queries.reshape(step_count, tile_rows, head_count, head_dim), grad_out.reshape(step_count, tile_rows, head_count, head_dim), selected.reshape(step_count, tile_rows, groups, -1), (jnp.arange(step_count) * tile_rows).astype(jnp.int32))
    zeros_init = jnp.zeros((groups, seq_len, head_dim), jnp.float32)
    (key_acc, value_acc), dquery = lax.scan(visit, (zeros_init, zeros_init), inputs)
    dquery = dquery.reshape(seq_len, head_count, head_dim)
    key_grad = key_acc.transpose(1, 0, 2).astype(jnp.bfloat16)
    value_grad = value_acc.transpose(1, 0, 2).astype(jnp.bfloat16)
    return (dquery, key_grad, value_grad)
```

```python
import functools
import math

import jax
import jax.numpy as jnp
from jax import lax
from jax.experimental import pallas as pl
from jax.experimental.pallas import tpu as pltpu
from jax.sharding import PartitionSpec as P

BLK = 64
NEG = -1e30
ID_ROWS = 16
LANES = 128
LOG2E = math.log2(math.e)
NT = (((1,), (1,)), ((), ()))
NN = (((1,), (0,)), ((), ()))


def attend(
    g, per_group, chunk_tokens, lo, hi, picked_ref, q_ref, do_ref, dq_ref, pool_ref, acc_ref
):
    tokens, _, dh = q_ref.shape
    own_rows = tokens
    keys = pool_ref.shape[1]
    slots = keys // BLK
    own_slots = own_rows // BLK
    scaling = 1.0 / math.sqrt(dh)
    log_scale = scaling * LOG2E
    rows = chunk_tokens * per_group
    shift = per_group.bit_length() - 1
    pool_k = pool_ref[0]
    pool_v = pool_ref[1]
    pool_kt = pool_k.T
    heads = slice(g * per_group, (g + 1) * per_group)

    @pl.loop(lo, hi)
    def _(c):
        t0 = pl.multiple_of(c * chunk_tokens, chunk_tokens)
        q = q_ref[pl.ds(t0, chunk_tokens), heads, :].reshape(rows, dh)
        do = do_ref[pl.ds(t0, chunk_tokens), heads, :].reshape(rows, dh)
        row_tok = t0 + (lax.broadcasted_iota(jnp.int32, (tokens, rows), 1) >> shift)
        tok = lax.broadcasted_iota(jnp.int32, (tokens, rows), 0)
        spread = jnp.where(row_tok == tok, 1.0, 0.0).astype(jnp.bfloat16)
        seen = lax.dot_general(picked_ref[g], spread, NN, preferred_element_type=jnp.float32)
        bias = (seen - 1.0) * (-NEG)
        s = lax.dot_general(pool_k, q, NT, preferred_element_type=jnp.float32)
        dp = lax.dot_general(pool_v, do, NT, preferred_element_type=jnp.float32)
        pieces = []
        for j in range(slots):
            piece = s[j * BLK : (j + 1) * BLK] + bias[j : j + 1]
            if j < own_slots:
                key_pos = j * BLK + lax.broadcasted_iota(jnp.int32, (BLK, rows), 0)
                causal = key_pos <= row_tok[:BLK]
                piece = jnp.where(causal, piece, NEG)
            pieces.append(piece)
        s = jnp.concatenate(pieces, axis=0)
        peak = jnp.max(s, axis=0, keepdims=True)
        e = jnp.exp2((s - peak) * log_scale)
        total = jnp.sum(e, axis=0, keepdims=True)
        weighted = jnp.sum(e * dp, axis=0, keepdims=True)
        inv = 1.0 / total
        inner = weighted * inv
        p = e * inv
        ds = (p * (dp - inner)).astype(jnp.bfloat16)
        p = p.astype(jnp.bfloat16)
        dqt = lax.dot_general(pool_kt, ds, NN, preferred_element_type=jnp.float32)
        dq = (dqt * scaling).T.astype(jnp.bfloat16)
        dq_ref[pl.ds(t0, chunk_tokens), heads, :] = dq.reshape(chunk_tokens, per_group, dh)
        dk = lax.dot_general(ds, q, NN, preferred_element_type=jnp.float32)
        dv = lax.dot_general(p, do, NN, preferred_element_type=jnp.float32)
        acc_ref[0] += dk.reshape(slots, BLK, dh)
        acc_ref[1] += dv.reshape(slots, BLK, dh)


def fill_tables(g, n, me, n_far, own_blocks, sel_ref, picked_ref, tab_ref):
    sel = sel_ref[g]
    tokens = sel.shape[1]
    shift = own_blocks.bit_length() - 1
    owner = sel >> shift
    block = sel & (own_blocks - 1)
    peers = lax.broadcasted_iota(jnp.int32, (n, tokens), 0)
    code = jnp.zeros((n, tokens), jnp.float32)
    for i in range(sel.shape[0]):
        mark = (block[i : i + 1] + 1).astype(jnp.float32)
        code = jnp.maximum(code, jnp.where(owner[i : i + 1] == peers, mark, 0.0))
    code = jnp.broadcast_to(jnp.max(code, axis=1, keepdims=True), (n, LANES))
    peers = lax.broadcasted_iota(jnp.int32, (n, LANES), 0)
    code = jnp.where(peers == me, 0.0, code)
    live = jnp.where(code > 0.0, 1.0, 0.0)
    before = lax.broadcasted_iota(jnp.int32, (n, n), 1) < lax.broadcasted_iota(jnp.int32, (n, n), 0)
    before = jnp.where(before, 1.0, 0.0).astype(jnp.bfloat16)
    slot = lax.dot_general(before, live.astype(jnp.bfloat16), NN, preferred_element_type=jnp.float32)
    far = jnp.maximum(code - 1.0, 0.0)
    lane = lax.broadcasted_iota(jnp.int32, (n, LANES), 1)
    kept = jnp.minimum(slot, float(n_far - 1))
    entry = jnp.where(lane == 0, kept, jnp.where(lane == 1, live, far))
    tab_ref[g, :n, :] = entry.astype(jnp.int32)
    peer = peers.astype(jnp.float32)
    now = me * own_blocks + (lax.broadcasted_iota(jnp.int32, (1, tokens), 1) >> BLK.bit_length() - 1)
    slots = picked_ref.shape[1]
    row = lax.broadcasted_iota(jnp.int32, (slots, tokens), 0)
    far_rows = tab_ref.shape[1] - n
    far_row = lax.broadcasted_iota(jnp.int32, (far_rows, LANES), 0)
    far_lane = lax.broadcasted_iota(jnp.int32, (far_rows, LANES), 1)
    far_entry = jnp.zeros((far_rows, LANES), jnp.float32)
    picked = jnp.zeros((slots, tokens), jnp.float32)
    for i in range(own_blocks + n_far):
        if i < own_blocks:
            ids = jnp.full((1, tokens), me * own_blocks + i, jnp.int32)
        else:
            hit = (live > 0.0) & (slot == float(i - own_blocks))
            who = jnp.max(jnp.where(hit, peer, -1.0), axis=0, keepdims=True)
            which = jnp.max(jnp.where(hit, far, 0.0), axis=0, keepdims=True)
            ids = jnp.max(who * own_blocks + which, axis=1, keepdims=True).astype(jnp.int32)
            ids = jnp.broadcast_to(ids, (1, tokens))
            here = jnp.where(far_lane == 0, jnp.maximum(who, 0.0), which)
            far_entry = jnp.where(far_row == i - own_blocks, here, far_entry)
        seen = jnp.max(jnp.where(sel == ids, 1.0, 0.0), axis=0, keepdims=True)
        seen = jnp.where(ids <= now, seen, 0.0)
        picked = jnp.where(row == i, seen, picked)
    tab_ref[g, n:, :] = far_entry.astype(jnp.int32)
    picked_ref[g] = picked.astype(jnp.bfloat16)


def fill_pool(g, n, n_far, tab, own_kv, gathered_ref, pool_ref):
    own_rows = own_kv.shape[2] * BLK
    pool_ref[:, :own_rows, :] = own_kv[g].reshape(2, own_rows, own_kv.shape[4])
    for s in range(n_far):
        owner = jnp.clip(tab[g, n + s, 0], 0, n - 1)
        block = jnp.clip(tab[g, n + s, 1], 0, own_kv.shape[2] - 1)
        lo = own_rows + s * BLK
        for kv in range(2):
            pool_ref[kv, lo : lo + BLK, :] = gathered_ref[owner, kv, block]


def fused_kernel(
    n, cols, n_far, chunk_tokens, groups,
    sel_ref, q_hbm, do_hbm, k_in, v_in, dq_ref, key_out, value_out, *scratch,
):
    per_bank = 9
    banks = [scratch[g * per_bank : (g + 1) * per_bank] for g in range(groups)]
    (
        picked_ref, tab_ref, tab, q_ref, do_ref, mix_ref, in_sem, pool_ref, mid_ref, col_send, y_send, sib_send, recv_sem,
        rs_sem, ry_send, ry_recv, rz_send, rz_recv, own_kv,
    ) = scratch[groups * per_bank :]
    depth = n // (2 * cols)
    chips = n // 2
    me = lax.axis_index("ctx")
    core = lax.rem(me, 2)
    chip = me // 2
    y = lax.rem(chip, cols)
    z = chip // cols
    sib = 2 * chip + 1 - core
    other_y = cols - 1 - y
    y_peer = 2 * (z * cols + other_y) + core
    own_blocks = own_kv.shape[2]
    own_rows = own_blocks * BLK
    dh = own_kv.shape[4]
    per_group = q_ref.shape[1] // groups
    chunks = q_ref.shape[0] // chunk_tokens
    scaling = 1.0 / math.sqrt(dh)

    def device(zz, yy, cc):
        return 2 * (zz * cols + yy) + cc

    def near(k):
        room = jnp.minimum(z, depth - 1 - z)
        step = jnp.where(lax.rem(k, 2) == 1, -((k + 1) // 2), k // 2)
        side = jnp.where(z < depth - 1 - z, k - room, room - k)
        return z + jnp.where(k <= 2 * room, step, side)

    def remote(src, dst, send, recv, peer):
        return pltpu.make_async_remote_copy(
            src_ref=src,
            dst_ref=dst,
            send_sem=send,
            recv_sem=recv,
            device_id={"ctx": peer},
            device_id_type=pl.DeviceIdType.MESH,
        )

    def col_copy(g, k):
        peer = device(near(k), y, core)
        return remote(
            own_kv.at[g], banks[g][0].at[me], col_send.at[g, k], recv_sem.at[g, me], peer
        )

    def own_copy(g, sem, peer):
        return remote(own_kv.at[g], banks[g][0].at[me], sem, recv_sem.at[g, me], peer)

    def pass_on(g, src, sem, peer):
        slot = banks[g][0].at[src]
        return remote(slot, slot, sem, recv_sem.at[g, src], peer)

    def await_piece(g, src):
        pass_on(g, src, sib_send.at[g, src], sib).wait_recv()

    def gather_start(g):
        if cols > 1:
            own_copy(g, y_send.at[g, z], y_peer).start()

        @pl.loop(1, depth)
        def _(k):
            col_copy(g, k).start()

        own_copy(g, sib_send.at[g, me], sib).start()

    def gather_column(g):
        @pl.loop(1, depth)
        def _(k):
            from_z = near(k)
            src = device(from_z, y, core)
            await_piece(g, src)
            if cols > 1:
                pass_on(g, src, y_send.at[g, from_z], y_peer).start()
            pass_on(g, src, sib_send.at[g, src], sib).start()

    def gather_across(g):
        if cols > 1:
            @pl.loop(0, depth)
            def _(k):
                src = device(jnp.where(k == 0, z, near(k)), other_y, core)
                await_piece(g, src)
                pass_on(g, src, sib_send.at[g, src], sib).start()

    def gather_end(g):
        @pl.loop(0, chips)
        def _(q):
            await_piece(g, 2 * q + 1 - core)

    def gather_drain(g):
        @pl.loop(1, depth)
        def _(k):
            col_copy(g, k).wait_send()

        if cols > 1:
            @pl.loop(0, depth)
            def _(k):
                pass_on(g, device(k, y, core), y_send.at[g, k], y_peer).wait_send()

        @pl.loop(0, chips)
        def _(q):
            src = 2 * q + core
            pass_on(g, src, sib_send.at[g, src], sib).wait_send()

    def sib_copy(g):
        return remote(banks[g][2], banks[g][3], rs_sem.at[g, 0], rs_sem.at[g, 1], sib)

    def y_copy(g, k):
        return remote(
            banks[g][4].at[k], banks[g][5].at[k], ry_send.at[g, k], ry_recv.at[g, k], y_peer
        )

    def z_copy(g, to_z):
        peer = device(to_z, y, core)
        return remote(
            banks[g][6].at[to_z], banks[g][7].at[z], rz_send.at[g, to_z], rz_recv.at[g, z], peer
        )

    def z_arrival(g, from_z):
        peer = device(from_z, y, core)
        return remote(
            banks[g][6].at[from_z], banks[g][7].at[from_z],
            rz_send.at[g, from_z], rz_recv.at[g, from_z], peer,
        )

    def far_part(g, dest, kv):
        return banks[g][1][kv, own_blocks + jnp.clip(tab[g, dest, 0], 0, n_far - 1)]

    def return_start(g):
        acc_ref, box = banks[g][1], banks[g][2]
        acc_ref[0] = acc_ref[0] * scaling

        @pl.loop(0, chips)
        def _(q):
            dest = 2 * q + 1 - core
            keep = tab[g, dest, 1].astype(jnp.float32)
            ids = jnp.full((ID_ROWS, dh), tab[g, dest, 2].astype(jnp.float32), jnp.float32)
            box[q, :ID_ROWS, :] = ids.astype(jnp.bfloat16)
            for kv in range(2):
                lo = ID_ROWS + kv * BLK
                box[q, lo : lo + BLK, :] = (far_part(g, dest, kv) * keep).astype(jnp.bfloat16)

        sib_copy(g).start()

    def merged(g, zz, yy):
        q = zz * cols + yy
        dest = 2 * q + core
        box = banks[g][3]
        which = box[q, :ID_ROWS, :].astype(jnp.float32)[:1]
        keep = tab[g, dest, 1].astype(jnp.float32)
        block = jnp.full((1, dh), tab[g, dest, 2].astype(jnp.float32), jnp.float32)
        for kv in range(2):
            lo = ID_ROWS + kv * BLK
            theirs = box[q, lo : lo + BLK, :].astype(jnp.float32)
            mine = far_part(g, dest, kv) * keep
            for b in range(own_blocks):
                yield kv, b, (
                    jnp.where(block == float(b), mine, 0.0)
                    + jnp.where(which == float(b), theirs, 0.0)
                )

    def return_across(g):
        sib_copy(g).wait_recv()
        if cols > 1:
            @pl.loop(0, depth)
            def _(k):
                zz = lax.rem(z + 1 + k, depth)
                for kv, b, part in merged(g, zz, other_y):
                    banks[g][4][zz, kv, b] = part.astype(jnp.bfloat16)
                y_copy(g, zz).start()

        @pl.loop(0, depth)
        def _(k):
            for kv, b, part in merged(g, k, y):
                mid_ref[k, kv, b] = part

    def return_column(g):
        @pl.loop(1, depth)
        def _(k):
            to_z = lax.rem(z + k, depth)
            total = mid_ref[to_z]
            if cols > 1:
                y_copy(g, to_z).wait_recv()
                total = total + banks[g][5][to_z].astype(jnp.float32)
            banks[g][6][to_z] = total.astype(jnp.bfloat16)
            z_copy(g, to_z).start()

        total = mid_ref[z] + banks[g][1][:, :own_blocks]
        if cols > 1:
            y_copy(g, z).wait_recv()
            total = total + banks[g][5][z].astype(jnp.float32)
        banks[g][8][...] = total

    def return_end(g):
        @pl.loop(1, depth)
        def _(k):
            from_z = lax.rem(z + depth - k, depth)
            z_arrival(g, from_z).wait_recv()
            banks[g][8][...] += banks[g][7][from_z].astype(jnp.float32)

        for kv in range(2):
            whole = banks[g][8][kv].reshape(own_rows, dh)
            mix_ref[kv, pl.ds(g, own_rows, stride=groups), :] = whole

    def return_drain(g):
        sib_copy(g).wait_send()
        if cols > 1:
            @pl.loop(0, depth)
            def _(k):
                y_copy(g, k).wait_send()

        @pl.loop(1, depth)
        def _(k):
            z_copy(g, lax.rem(z + k, depth)).wait_send()

    barrier = pltpu.get_barrier_semaphore()

    def greet(peer):
        pl.semaphore_signal(
            barrier, inc=1, device_id={"ctx": peer}, device_id_type=pl.DeviceIdType.MESH
        )

    @pl.loop(1, depth)
    def _(k):
        greet(device(lax.rem(z + k, depth), y, core))

    if cols > 1:
        greet(y_peer)
    greet(sib)
    loads = [
        pltpu.make_async_copy(q_hbm, q_ref, in_sem.at[0]),
        pltpu.make_async_copy(do_hbm, do_ref, in_sem.at[1]),
    ]
    for load in loads:
        load.start()
    for kv, source in enumerate((k_in, v_in)):
        mix_ref[kv, : own_rows * groups] = source[...].astype(jnp.float32)
        for g in range(groups):
            rows = mix_ref[kv, pl.ds(g, own_rows, stride=groups), :].astype(jnp.bfloat16)
            own_kv[g, kv] = rows.reshape(own_blocks, BLK, dh)
    pl.semaphore_wait(barrier, depth + cols - 1)
    for g in range(groups):
        gather_start(g)
    for g in range(groups):
        fill_tables(g, n, me, n_far, own_blocks, sel_ref, picked_ref, tab_ref)
    to_scalars = pltpu.make_async_copy(tab_ref, tab, in_sem.at[2])
    to_scalars.start()
    for g in range(groups):
        banks[g][1][...] = jnp.zeros_like(banks[g][1])
    to_scalars.wait()
    for load in loads:
        load.wait()
    gather_column(0)
    gather_across(0)
    gather_end(0)
    for g in range(groups):
        first, last = [], []
        if g + 1 < groups:
            first.append(functools.partial(gather_column, g + 1))
            last.append(functools.partial(gather_across, g + 1))
        if g > 0:
            first.append(functools.partial(return_across, g - 1))
            last.append(functools.partial(return_column, g - 1))
        fill_pool(g, n, n_far, tab, own_kv, banks[g][0], pool_ref)
        cuts = sorted({0, min(1, chunks), chunks // 2, chunks})
        for i in range(len(cuts) - 1):
            attend(
                g, per_group, chunk_tokens, cuts[i], cuts[i + 1],
                picked_ref, q_ref, do_ref, dq_ref, pool_ref, banks[g][1],
            )
            for step in (first if i == 0 else last if i == len(cuts) - 2 else []):
                step()
        if g + 1 < groups:
            gather_end(g + 1)
        return_start(g)
    final = groups - 1
    return_across(final)
    return_column(final)
    for g in range(groups):
        return_end(g)
    for g in range(groups):
        gather_drain(g)
        return_drain(g)
    key_out[...] = mix_ref[0, : own_rows * groups].astype(jnp.bfloat16)
    value_out[...] = mix_ref[1, : own_rows * groups].astype(jnp.bfloat16)


def store_kernel(*refs):
    count = (len(refs) - 1) // 2
    sem = refs[-1]
    copies = [
        pltpu.make_async_copy(refs[i], refs[count + i], sem.at[i]) for i in range(count)
    ]
    for copy in copies:
        copy.start()
    for copy in copies:
        copy.wait()


def store(arrays):
    return pl.pallas_call(
        store_kernel,
        out_shape=tuple(jax.ShapeDtypeStruct(a.shape, a.dtype) for a in arrays),
        in_specs=[pl.BlockSpec(memory_space=pltpu.VMEM)] * len(arrays),
        out_specs=(pl.BlockSpec(memory_space=pl.ANY),) * len(arrays),
        scratch_shapes=[pltpu.SemaphoreType.DMA((len(arrays),))],
    )(*arrays)


def columns_of(mesh, n):
    spots = [getattr(d, "coords", None) for d in mesh.devices.reshape(-1, n)[0]]
    if None in spots or n % 2:
        return 1
    cols = sum(spot[2] == spots[0][2] for spot in spots) // 2
    return 2 if cols == 2 and n % 4 == 0 else 1


def local(cols, queries, keys, values, grad_out, selected):
    tokens, head_count, dh = queries.shape
    groups = keys.shape[1]
    own_blocks = tokens // BLK
    n = lax.axis_size("ctx")
    depth = n // (2 * cols)
    fetched = min(n - 2, max(selected.shape[2] - own_blocks, 4)) + 1
    slots = -(-(own_blocks + fetched) // 16) * 16
    far_rows = -(-fetched // 8) * 8
    pool_rows = (own_blocks + fetched) * BLK
    chosen = selected.transpose(1, 2, 0)
    piece = (2, own_blocks, BLK, dh)
    vmem = pl.BlockSpec(memory_space=pltpu.VMEM)
    any_spec = pl.BlockSpec(memory_space=pl.ANY)
    bank = [
        pltpu.VMEM((n,) + piece, jnp.bfloat16),
        pltpu.VMEM((2, pool_rows // BLK, BLK, dh), jnp.float32),
        pltpu.VMEM((n // 2, ID_ROWS + 2 * BLK, dh), jnp.bfloat16),
        pltpu.VMEM((n // 2, ID_ROWS + 2 * BLK, dh), jnp.bfloat16),
        pltpu.VMEM((depth,) + piece, jnp.bfloat16),
        pltpu.VMEM((depth,) + piece, jnp.bfloat16),
        pltpu.VMEM((depth,) + piece, jnp.bfloat16),
        pltpu.VMEM((depth,) + piece, jnp.bfloat16),
        pltpu.VMEM(piece, jnp.float32),
    ]
    dma = pltpu.SemaphoreType.DMA
    dq, key_grad, value_grad = pl.pallas_call(
        functools.partial(fused_kernel, n, cols, fetched, min(tokens, 32), groups),
        out_shape=(
            pltpu.VMEM(queries.shape, jnp.bfloat16),
            pltpu.VMEM((tokens * groups, dh), jnp.bfloat16),
            pltpu.VMEM((tokens * groups, dh), jnp.bfloat16),
        ),
        in_specs=[vmem, any_spec, any_spec, vmem, vmem],
        out_specs=(vmem, vmem, vmem),
        scratch_shapes=bank * groups + [
            pltpu.VMEM((groups, slots, tokens), jnp.bfloat16),
            pltpu.VMEM((groups, n + far_rows, LANES), jnp.int32),
            pltpu.SMEM((groups, n + far_rows, LANES), jnp.int32),
            pltpu.VMEM(queries.shape, jnp.bfloat16),
            pltpu.VMEM(queries.shape, jnp.bfloat16),
            pltpu.VMEM((2, tokens * groups + 8, dh), jnp.float32),
            dma((3,)),
            pltpu.VMEM((2, pool_rows, dh), jnp.bfloat16),
            pltpu.VMEM((depth,) + piece, jnp.float32),
            dma((groups, depth)),
            dma((groups, depth)),
            dma((groups, n)),
            dma((groups, n)),
            dma((groups, 2)),
            dma((groups, depth)),
            dma((groups, depth)),
            dma((groups, depth)),
            dma((groups, depth)),
            pltpu.VMEM((groups,) + piece, jnp.bfloat16),
        ],
        compiler_params=pltpu.CompilerParams(collective_id=0, has_side_effects=True),
    )(
        chosen,
        queries,
        grad_out,
        keys.reshape(tokens * groups, dh),
        values.reshape(tokens * groups, dh),
    )
    held = (dq, key_grad, value_grad)
    held = [pltpu.with_memory_space_constraint(a, pltpu.VMEM) for a in held]
    dq, key_grad, value_grad = store(held)
    return dq, key_grad.reshape(keys.shape), value_grad.reshape(values.shape)


def solution(mesh):
    spec = P(("rep", "ctx"), None, None)
    cols = columns_of(mesh, mesh.shape["ctx"])
    return jax.shard_map(
        functools.partial(local, cols),
        mesh=mesh,
        in_specs=(spec,) * 5,
        out_specs=(spec,) * 3,
        check_vma=False,
    )
```

```python
import functools
import math

import jax
import jax.numpy as jnp
from jax import lax
from jax.experimental import pallas as pl
from jax.experimental.pallas import tpu as pltpu
from jax.sharding import PartitionSpec as P

BLK = 64
NEG = -1e30
BAND = 3
LANES = 128
LOG2E = math.log2(math.e)
NT = (((1,), (1,)), ((), ()))
NN = (((1,), (0,)), ((), ()))


def rows_of(ref, c, chunk_tokens, heads):
    part = ref[c * chunk_tokens : (c + 1) * chunk_tokens, heads, :]
    return part.reshape(part.shape[0] * part.shape[1], part.shape[2])


def bands(total):
    step = BLK * BAND
    return [(lo, min(lo + step, total)) for lo in range(0, total, step)]


def fold(x, op):
    return op(x.reshape(x.shape[0] // 8, 8, x.shape[1]), axis=0)


def fill_bias(picked, per_group, chunk_tokens, bias_ref, own_bias_ref):
    tokens = picked.shape[1]
    rows = chunk_tokens * per_group
    shift = per_group.bit_length() - 1

    @pl.loop(0, tokens // chunk_tokens)
    def _(c):
        row_tok = c * chunk_tokens + (lax.broadcasted_iota(jnp.int32, (tokens, rows), 1) >> shift)
        tok = lax.broadcasted_iota(jnp.int32, (tokens, rows), 0)
        spread = jnp.where(row_tok == tok, 1.0, 0.0).astype(jnp.bfloat16)
        seen = lax.dot_general(picked, spread, NN, preferred_element_type=jnp.float32)
        bias = (seen - 1.0) * (-NEG)
        bias_ref[c] = bias
        for j in range(tokens // BLK):
            at = slice(j * BLK, (j + 1) * BLK)
            own_bias_ref[c, at] = jnp.where(tok[at] <= row_tok[at], bias[j : j + 1], NEG)


class Weigh:
    def __init__(self, heads, chunk_tokens, bias, own_bias, q_ref, do_ref, keys, s_ref, e_ref, acc_ref):
        self.__dict__.update(locals())
        self.peak, self.inv = {}, {}

    def scores(self, c):
        tokens, _, dh = self.q_ref.shape
        q = rows_of(self.q_ref, c, self.chunk_tokens, self.heads)
        peak = None
        for lo, hi in bands(self.keys.shape[0]):
            s = lax.dot_general(self.keys[lo:hi], q, NT, preferred_element_type=jnp.float32)
            for j in range(lo // BLK, hi // BLK):
                part = s[j * BLK - lo : (j + 1) * BLK - lo]
                if j < tokens // BLK:
                    part = part + self.own_bias[c, j * BLK : (j + 1) * BLK]
                else:
                    part = part + self.bias[c, j : j + 1]
                self.s_ref[c % 2, j * BLK : (j + 1) * BLK] = part
                top = fold(part, jnp.max)
                peak = top if peak is None else jnp.maximum(peak, top)
            yield
        log_scale = LOG2E / math.sqrt(dh)
        self.peak[c] = jnp.max(peak, axis=0, keepdims=True) * log_scale

    def exponents(self, c):
        dh = self.q_ref.shape[2]
        log_scale = LOG2E / math.sqrt(dh)
        total = None
        for lo, hi in bands(self.keys.shape[0]):
            for j in range(lo // BLK, hi // BLK):
                at = slice(j * BLK, (j + 1) * BLK)
                e = jnp.exp2(self.s_ref[c % 2, at] * log_scale - self.peak[c])
                self.e_ref[c, at] = e
                part = fold(e, jnp.sum)
                total = part if total is None else total + part
            yield
        self.inv[c] = 1.0 / jnp.sum(total, axis=0, keepdims=True)

    def products(self, c):
        do = rows_of(self.do_ref, c, self.chunk_tokens, self.heads)
        for lo, hi in bands(self.keys.shape[0]):
            p = self.e_ref[c, lo:hi] * self.inv[c]
            self.e_ref[c, lo:hi] = p
            dv = lax.dot_general(p.astype(jnp.bfloat16), do, NN, preferred_element_type=jnp.float32)
            dv = dv.reshape((hi - lo) // BLK, BLK, dv.shape[1])
            at = slice(lo // BLK, hi // BLK)
            self.acc_ref[at] = dv if c == 0 else self.acc_ref[at] + dv
            yield


class Slope:
    def __init__(self, heads, chunk_tokens, q_ref, do_ref, values, s_ref, e_ref, ds_ref, acc_ref):
        self.__dict__.update(locals())
        self.inner = {}

    def scores(self, c):
        do = rows_of(self.do_ref, c, self.chunk_tokens, self.heads)
        total = None
        for lo, hi in bands(self.values.shape[0]):
            dp = lax.dot_general(self.values[lo:hi], do, NT, preferred_element_type=jnp.float32)
            for j in range(lo // BLK, hi // BLK):
                part = dp[j * BLK - lo : (j + 1) * BLK - lo]
                self.s_ref[c % 2, j * BLK : (j + 1) * BLK] = part
                part = fold(part * self.e_ref[c, j * BLK : (j + 1) * BLK], jnp.sum)
                total = part if total is None else total + part
            yield
        self.inner[c] = jnp.sum(total, axis=0, keepdims=True)

    def products(self, c):
        q = rows_of(self.q_ref, c, self.chunk_tokens, self.heads)
        for lo, hi in bands(self.values.shape[0]):
            dp = self.s_ref[c % 2, lo:hi]
            ds = (self.e_ref[c, lo:hi] * (dp - self.inner[c])).astype(jnp.bfloat16)
            self.ds_ref[c, lo:hi] = ds
            dk = lax.dot_general(ds, q, NN, preferred_element_type=jnp.float32)
            dk = dk.reshape((hi - lo) // BLK, BLK, dk.shape[1])
            at = slice(lo // BLK, hi // BLK)
            self.acc_ref[at] = dk if c == 0 else self.acc_ref[at] + dk
            yield


def side_by_side(parts):
    parts = list(parts)
    while parts:
        parts = [part for part in parts if next(part, parts) is None]


def pipelined(phases, chunks, between):
    depth = len(phases)
    for t in range(chunks + depth - 1):
        live = [(i, t - i) for i in range(depth) if 0 <= t - i < chunks]
        side_by_side(phases[i](c) for i, c in reversed(live))
        between(t)


def query_grad(c, heads, chunk_tokens, keys_t, ds_ref, dq_ref):
    dh = keys_t.shape[0]
    t0 = pl.multiple_of(c * chunk_tokens, chunk_tokens)
    dqt = lax.dot_general(keys_t, ds_ref[c], NN, preferred_element_type=jnp.float32)
    dq = (dqt * (1.0 / math.sqrt(dh))).T.astype(jnp.bfloat16)
    per_group = heads.stop - heads.start
    dq_ref[pl.ds(t0, chunk_tokens), heads, :] = dq.reshape(chunk_tokens, per_group, dh)


def fill_tables(g, n, me, n_far, own_blocks, sel_ref, picked_ref, tab_ref):
    sel = sel_ref[g]
    tokens = sel.shape[1]
    shift = own_blocks.bit_length() - 1
    owner = sel >> shift
    block = sel & (own_blocks - 1)
    peers = lax.broadcasted_iota(jnp.int32, (n, tokens), 0)
    code = jnp.zeros((n, tokens), jnp.float32)
    for i in range(sel.shape[0]):
        mark = (block[i : i + 1] + 1).astype(jnp.float32)
        code = jnp.maximum(code, jnp.where(owner[i : i + 1] == peers, mark, 0.0))
    code = jnp.broadcast_to(jnp.max(code, axis=1, keepdims=True), (n, LANES))
    peers = lax.broadcasted_iota(jnp.int32, (n, LANES), 0)
    code = jnp.where(peers == me, 0.0, code)
    live = jnp.where(code > 0.0, 1.0, 0.0)
    before = lax.broadcasted_iota(jnp.int32, (n, n), 1) < lax.broadcasted_iota(jnp.int32, (n, n), 0)
    before = jnp.where(before, 1.0, 0.0).astype(jnp.bfloat16)
    slot = lax.dot_general(before, live.astype(jnp.bfloat16), NN, preferred_element_type=jnp.float32)
    far = jnp.maximum(code - 1.0, 0.0)
    lane = lax.broadcasted_iota(jnp.int32, (n, LANES), 1)
    kept = jnp.minimum(slot, float(n_far - 1))
    entry = jnp.where(lane == 0, kept, jnp.where(lane == 1, live, far))
    tab_ref[g, :n, :] = entry.astype(jnp.int32)
    peer = peers.astype(jnp.float32)
    now = me * own_blocks + (lax.broadcasted_iota(jnp.int32, (1, tokens), 1) >> BLK.bit_length() - 1)
    slots = picked_ref.shape[1]
    row = lax.broadcasted_iota(jnp.int32, (slots, tokens), 0)
    far_rows = tab_ref.shape[1] - n
    far_row = lax.broadcasted_iota(jnp.int32, (far_rows, LANES), 0)
    far_lane = lax.broadcasted_iota(jnp.int32, (far_rows, LANES), 1)
    far_entry = jnp.zeros((far_rows, LANES), jnp.float32)
    picked = jnp.zeros((slots, tokens), jnp.float32)
    for i in range(own_blocks + n_far):
        if i < own_blocks:
            ids = jnp.full((1, tokens), me * own_blocks + i, jnp.int32)
        else:
            hit = (live > 0.0) & (slot == float(i - own_blocks))
            who = jnp.max(jnp.where(hit, peer, -1.0), axis=0, keepdims=True)
            which = jnp.max(jnp.where(hit, far, 0.0), axis=0, keepdims=True)
            ids = jnp.max(who * own_blocks + which, axis=1, keepdims=True).astype(jnp.int32)
            ids = jnp.broadcast_to(ids, (1, tokens))
            here = jnp.where(far_lane == 0, jnp.maximum(who, 0.0), which)
            far_entry = jnp.where(far_row == i - own_blocks, here, far_entry)
        seen = jnp.max(jnp.where(sel == ids, 1.0, 0.0), axis=0, keepdims=True)
        seen = jnp.where(ids <= now, seen, 0.0)
        picked = jnp.where(row == i, seen, picked)
    tab_ref[g, n:, :] = far_entry.astype(jnp.int32)
    picked_ref[g] = picked.astype(jnp.bfloat16)


def fused_kernel(
    n, cols, n_far, chunk_tokens, groups,
    sel_hbm, q_hbm, do_hbm, k_hbm, v_hbm, dq_ref, key_out, value_out,
    sel_ref, q_ref, do_ref, raw_ref, mix_ref, own, pool, acc, s_ref, e_ref, bias_ref, own_bias_ref, ds_ref,
    picked_ref, tab_ref, mate_tab_ref, tab, box, box_in, z_box, z_in, total_ref,
    in_sem, tab_sem, zs, zr, ys, yr, ss, sr, box_send, box_recv, rz_send, rz_recv, *banks,
):
    gaths, mate_tabs = list(banks[: 2 * groups]), list(banks[2 * groups :])
    depth = n // (2 * cols)
    chips = n // 2
    me = lax.axis_index("ctx")
    core = lax.rem(me, 2)
    chip = me // 2
    y = lax.rem(chip, cols)
    z = chip // cols
    sib = 2 * chip + 1 - core
    other_y = cols - 1 - y
    y_peer = 2 * (z * cols + other_y) + core
    own_blocks = own.shape[1]
    own_rows = own_blocks * BLK
    dh = own.shape[3]
    per_group = q_ref.shape[1] // groups
    chunks = q_ref.shape[0] // chunk_tokens
    scaling = 1.0 / math.sqrt(dh)
    pieces = 2 * groups
    near_max = depth - 1

    def device(zz, yy, cc):
        return 2 * (zz * cols + yy) + cc

    def near(k):
        room = jnp.minimum(z, depth - 1 - z)
        step = jnp.where(lax.rem(k, 2) == 1, -((k + 1) // 2), k // 2)
        side = jnp.where(z < depth - 1 - z, k - room, room - k)
        return z + jnp.where(k <= 2 * room, step, side)

    def remote(src, dst, send, recv, peer):
        return pltpu.make_async_remote_copy(
            src_ref=src,
            dst_ref=dst,
            send_sem=send,
            recv_sem=recv,
            device_id={"ctx": peer},
            device_id_type=pl.DeviceIdType.MESH,
        )

    def direct(p):
        return p < 2

    def z_send(p, src, from_z, to_z):
        dst = gaths[p].at[core, from_z * cols + y]
        return remote(src, dst, zs.at[p], zr.at[p, from_z], device(to_z, y, core))

    def z_wait(p, from_z):
        spot = gaths[p].at[core, from_z * cols + y]
        remote(spot, spot, zs.at[p], zr.at[p, from_z], y_peer if cols > 1 else sib).wait_recv()

    def y_send(p, src, from_z):
        dst = gaths[p].at[core, from_z * cols + y]
        return remote(src, dst, ys.at[p], yr.at[p, from_z], y_peer)

    def y_wait(p, from_z):
        spot = gaths[p].at[core, from_z * cols + other_y]
        remote(spot, spot, ys.at[p], yr.at[p, from_z], y_peer).wait_recv()

    def sib_send(p, src, q):
        return remote(src, gaths[p].at[core, q], ss.at[p], sr.at[p], sib)

    def gather_start(p):
        if cols > 1:
            y_send(p, own.at[p], z).start()

        if direct(p):
            @pl.loop(1, depth)
            def _(k):
                z_send(p, own.at[p], z, near(depth - k)).start()
        else:
            for to_z in (z - 1, z + 1):
                @pl.when((to_z >= 0) & (to_z < depth))
                def _():
                    z_send(p, own.at[p], z, to_z).start()

        sib_send(p, own.at[p], chip).start()

    def span(i):
        return 1 + i * near_max // 3, 1 + (i + 1) * near_max // 3

    def each_at(d, visit):
        for side in (-1, 1):
            from_z = z + side * d

            @pl.when((from_z >= 0) & (from_z < depth))
            def _():
                visit(from_z, z - side)

    def z_step(p, i):
        lo, hi = span(i)

        def visit(from_z, to_z):
            q = from_z * cols + y
            spot = gaths[p].at[core, q]
            z_wait(p, from_z)
            if not direct(p):
                @pl.when((to_z >= 0) & (to_z < depth))
                def _():
                    z_send(p, spot, from_z, to_z).start()


            if cols > 1:
                y_send(p, spot, from_z).start()
            sib_send(p, spot, q).start()

        @pl.loop(lo, hi)
        def _(d):
            each_at(d, visit)

    def y_step(p, i):
        if cols == 1:
            return

        def visit(from_z, to_z):
            q = from_z * cols + other_y
            y_wait(p, from_z)
            sib_send(p, gaths[p].at[core, q], q).start()

        if i == 0:
            visit(z, z)
        else:
            lo, hi = span(i - 1)

            @pl.loop(lo, hi)
            def _(d):
                each_at(d, visit)

    def gather_end(p):
        spot = gaths[p].at[1 - core]
        remote(spot, spot, ss.at[p], sr.at[p], sib).wait_recv()

    def z_drain(p, count):
        @pl.loop(0, count)
        def _(k):
            z_send(p, own.at[p], z, z).wait_send()

    def gather_drain(p):
        spot = gaths[p].at[core]
        remote(spot, spot, ss.at[p], sr.at[p], sib).wait_send()
        if direct(p):
            z_drain(p, depth - 1)
        else:
            for more, count in ((z > 0, depth - z), (z < depth - 1, z + 1)):
                @pl.when(more)
                def _():
                    z_drain(p, count)

        if cols > 1:
            part = gaths[p].at[core, pl.ds(0, depth)]
            remote(part, part, ys.at[p], yr.at[p, z], y_peer).wait_send()

    def fill_pool(p):
        g = p // 2
        pool[p, :own_rows, :] = own[p].reshape(own_rows, dh)
        for s in range(n_far):
            owner = jnp.clip(tab[g, n + s, 0], 0, n - 1)
            block = jnp.clip(tab[g, n + s, 1], 0, own_blocks - 1)
            lo = own_rows + s * BLK
            pool[p, lo : lo + BLK, :] = gaths[p][owner & 1, owner >> 1, block]

    mates = [(y, 1 - core)] + ([(other_y, core), (other_y, 1 - core)] if cols > 1 else [])

    def mate_copy(p, m, zz):
        return remote(
            box.at[p, m, zz], box_in.at[p, m, zz], box_send.at[p, m], box_recv.at[p, m, zz],
            device(z, *mates[m]),
        )

    def z_copy(p, to_z):
        return remote(
            z_box.at[p, to_z], z_in.at[p, z], rz_send.at[p], rz_recv.at[p], device(to_z, y, core)
        )

    def factor(p):
        return scaling if p % 2 == 0 else 1.0

    def far_part(p, dest):
        return acc[p, own_blocks + jnp.clip(tab[p // 2, dest, 0], 0, n_far - 1)]

    def far_first(k):
        return jnp.where(k == depth, z, near(jnp.maximum(depth - k, 1)))

    def return_start(p):
        g = p // 2

        @pl.loop(1, depth + 1)
        def _(k):
            zz = far_first(k)
            for m, (yy, cc) in enumerate(mates):
                dest = device(zz, yy, cc)
                keep = tab[g, dest, 1].astype(jnp.float32) * factor(p)
                box[p, m, zz] = (far_part(p, dest) * keep).astype(jnp.bfloat16)
            for m in range(len(mates)):
                mate_copy(p, m, zz).start()

    def merged(p, zz):
        g = p // 2
        dest = device(zz, y, core)
        for m in range(len(mates)):
            mate_copy(p, m, zz).wait_recv()
        parts = [far_part(p, dest) * (tab[g, dest, 1].astype(jnp.float32) * factor(p))]
        tables = [tab] + mate_tabs
        for m in range(len(mates)):
            parts.append(box_in[p, m, zz].astype(jnp.float32))
        for b in range(own_blocks):
            total = None
            for table, part in zip(tables, parts):
                share = part * jnp.where(table[g, dest, 2] == b, 1.0, 0.0)
                total = share if total is None else total + share
            yield b, total

    def return_column(p, i):
        lo, hi = span(i)

        @pl.loop(lo, hi)
        def _(k):
            to_z = far_first(k)
            for b, part in merged(p, to_z):
                z_box[p, to_z, b] = part.astype(jnp.bfloat16)
            z_copy(p, to_z).start()

    def return_own(p):
        for b, part in merged(p, z):
            total_ref[p, b] = part + acc[p, b] * factor(p)

    def return_end(p):
        part = z_in.at[p, pl.ds(0, depth - 1)]
        remote(part, part, rz_send.at[p], rz_recv.at[p], sib).wait_recv()

        @pl.loop(1, depth)
        def _(k):
            from_z = near(k)
            total_ref[p] += z_in[p, from_z].astype(jnp.float32)

        whole = total_ref[p].reshape(own_rows, dh)
        mix_ref[p % 2, pl.ds(p // 2, own_rows, stride=groups), :] = whole

    def return_drain(p):
        for m in range(len(mates)):
            part = box.at[p, m]
            remote(part, part, box_send.at[p, m], box_recv.at[p, m, 0], sib).wait_send()
        part = z_box.at[p, pl.ds(0, depth - 1)]
        remote(part, part, rz_send.at[p], rz_recv.at[p], sib).wait_send()

    barrier = pltpu.get_barrier_semaphore()

    def greet(peer):
        pl.semaphore_signal(
            barrier, inc=1, device_id={"ctx": peer}, device_id_type=pl.DeviceIdType.MESH
        )

    @pl.loop(1, depth)
    def _(k):
        greet(device(near(k), y, core))

    for yy, cc in mates:
        greet(device(z, yy, cc))
    loads = [
        pltpu.make_async_copy(src, dst, in_sem.at[i])
        for i, (src, dst) in enumerate([
            (k_hbm, raw_ref.at[0]), (v_hbm, raw_ref.at[1]), (sel_hbm, sel_ref), (q_hbm, q_ref), (do_hbm, do_ref),
        ])
    ]
    for load in loads:
        load.start()
    for kv in range(2):
        loads[kv].wait()
        mix_ref[kv, : own_rows * groups] = raw_ref[kv].astype(jnp.float32)
        for g in range(groups):
            rows = mix_ref[kv, pl.ds(g, own_rows, stride=groups), :].astype(jnp.bfloat16)
            own[2 * g + kv] = rows.reshape(own_blocks, BLK, dh)
    pl.semaphore_wait(barrier, depth - 1 + len(mates))
    for p in range(pieces):
        gather_start(p)
    loads[2].wait()
    for g in range(groups):
        fill_tables(g, n, me, n_far, own_blocks, sel_ref, picked_ref, tab_ref)
    to_scalars = pltpu.make_async_copy(tab_ref, tab, in_sem.at[5])
    to_scalars.start()
    to_mates = [
        remote(
            tab_ref, mate_tab_ref.at[m], tab_sem.at[0, m], tab_sem.at[1, m], device(z, yy, cc)
        )
        for m, (yy, cc) in enumerate(mates)
    ]
    for copy in to_mates:
        copy.start()
    for g in range(groups):
        fill_bias(picked_ref[g], per_group, chunk_tokens, bias_ref.at[g], own_bias_ref.at[g])
    to_scalars.wait()
    loads[3].wait()
    loads[4].wait()

    def run(steps):
        for name, *args in steps:
            {
                "z": z_step, "y": y_step, "end": gather_end, "pool": fill_pool,
                "start": return_start, "column": return_column,
                "own": return_own, "done": return_end,
            }[name](*args)

    K0, V0, K1, V1 = range(4) if groups == 2 else (0, 1, None, None)

    def stage(body, plan):
        @pl.loop(0, chunks)
        def _(c):
            body(c)
            for i, steps in enumerate(plan):
                @pl.when(c == min(i, chunks - 1))
                def _():
                    run(steps)

    def heads(g):
        return slice(g * per_group, (g + 1) * per_group)

    def between(plan):
        return lambda t: run(plan[t] if t < len(plan) else [])

    def weigh_stage(g, plan):
        work = Weigh(
            heads(g), chunk_tokens, bias_ref.at[g], own_bias_ref.at[g], q_ref, do_ref,
            pool.at[2 * g], s_ref, e_ref, acc.at[2 * g + 1],
        )
        pipelined([work.scores, work.exponents, work.products], chunks, between(plan))

    def slope_stage(g, plan):
        work = Slope(
            heads(g), chunk_tokens, q_ref, do_ref, pool.at[2 * g + 1], s_ref, e_ref,
            ds_ref.at[g], acc.at[2 * g],
        )
        pipelined([work.scores, work.products], chunks, between(plan))

    def query_stage(g, plan):
        keys_t = pool[2 * g].T
        stage(lambda c: query_grad(c, heads(g), chunk_tokens, keys_t, ds_ref.at[g], dq_ref), plan)

    run([("y", K0, 0), ("z", K0, 0), ("z", K0, 1), ("z", K0, 2), ("y", V0, 0)])
    for copy in to_mates:
        copy.wait_recv()
    backs = [
        pltpu.make_async_copy(mate_tab_ref.at[m], mate_tabs[m], in_sem.at[6 + m])
        for m in range(len(mates))
    ]
    for copy in backs:
        copy.start()
    run([("y", K1, 0), ("y", V1, 0), ("z", V0, 0), ("z", V0, 1), ("z", V0, 2), ("z", K1, 0),
         ("z", V1, 0), ("y", K0, 1), ("y", K0, 2), ("y", K0, 3), ("end", K0), ("pool", K0)])
    for copy in backs:
        copy.wait()
    weigh_stage(0, [
        [("z", K1, 1), ("y", V0, 1)],
        [("z", V1, 1), ("y", V0, 2)],
        [("y", V0, 3)],
        [("z", K1, 2), ("y", K1, 1)],
        [("z", V1, 2), ("y", V1, 1)],
    ])
    run([("start", V0), ("end", V0), ("pool", V0)])
    slope_stage(0, [
        [],
        [("y", K1, 2)],
        [("y", V1, 2)],
        [("y", K1, 3)],
    ])
    run([("start", K0), ("end", K1), ("pool", K1)])
    weigh_stage(1, [
        [],
        [("y", V1, 3)],
        [("column", V0, 0), ("column", V0, 1), ("column", V0, 2)],
        [("own", V0)],
        [("column", K0, 0), ("column", K0, 1), ("column", K0, 2)],
    ])
    run([("start", V1), ("own", K0), ("end", V1), ("pool", V1)])
    slope_stage(1, [])
    run([("start", K1)])
    query_stage(0, [
        [],
        [],
        [],
        [("column", V1, 0), ("column", V1, 1), ("column", V1, 2)],
    ])
    query_stage(1, [
        [],
        [("done", V0)],
        [("own", V1)],
        [("column", K1, 0)],
    ])
    run([("column", K1, 1), ("column", K1, 2), ("done", K0), ("own", K1), ("done", V1), ("done", K1)])
    for copy in to_mates:
        copy.wait_send()
    for p in range(pieces):
        gather_drain(p)
        return_drain(p)
    key_out[...] = mix_ref[0, : own_rows * groups].astype(jnp.bfloat16)
    value_out[...] = mix_ref[1, : own_rows * groups].astype(jnp.bfloat16)


def store_kernel(*refs):
    count = (len(refs) - 1) // 2
    sem = refs[-1]
    copies = [
        pltpu.make_async_copy(refs[i], refs[count + i], sem.at[i]) for i in range(count)
    ]
    for copy in copies:
        copy.start()
    for copy in copies:
        copy.wait()


def store(arrays):
    return pl.pallas_call(
        store_kernel,
        out_shape=tuple(jax.ShapeDtypeStruct(a.shape, a.dtype) for a in arrays),
        in_specs=[pl.BlockSpec(memory_space=pltpu.VMEM)] * len(arrays),
        out_specs=(pl.BlockSpec(memory_space=pl.ANY),) * len(arrays),
        scratch_shapes=[pltpu.SemaphoreType.DMA((len(arrays),))],
    )(*arrays)


def columns_of(mesh, n):
    spots = [getattr(d, "coords", None) for d in mesh.devices.reshape(-1, n)[0]]
    if None in spots or n % 2:
        return 1
    cols = sum(spot[2] == spots[0][2] for spot in spots) // 2
    return 2 if cols == 2 and n % 4 == 0 else 1


def local(cols, queries, keys, values, grad_out, selected):
    tokens, head_count, dh = queries.shape
    groups = keys.shape[1]
    own_blocks = tokens // BLK
    n = lax.axis_size("ctx")
    depth = n // (2 * cols)
    chips = n // 2
    pieces = 2 * groups
    fetched = min(n - 2, max(selected.shape[2] - own_blocks, 4)) + 1
    slots = -(-(own_blocks + fetched) // 16) * 16
    far_rows = -(-fetched // 8) * 8
    pool_blocks = own_blocks + fetched
    pool_rows = pool_blocks * BLK
    chunk_tokens = min(tokens, 32)
    chunks = tokens // chunk_tokens
    rows = chunk_tokens * head_count // groups
    chosen = selected.transpose(1, 2, 0)
    mates = 3 if cols > 1 else 1
    any_spec = pl.BlockSpec(memory_space=pl.ANY)
    vmem = pl.BlockSpec(memory_space=pltpu.VMEM)
    dma = pltpu.SemaphoreType.DMA
    bf16, f32, i32 = jnp.bfloat16, jnp.float32, jnp.int32
    held = pl.pallas_call(
        functools.partial(fused_kernel, n, cols, fetched, chunk_tokens, groups),
        out_shape=(
            pltpu.VMEM(queries.shape, bf16),
            pltpu.VMEM((tokens * groups, dh), bf16),
            pltpu.VMEM((tokens * groups, dh), bf16),
        ),
        in_specs=[any_spec] * 5,
        out_specs=(vmem, vmem, vmem),
        scratch_shapes=[
            pltpu.VMEM(chosen.shape, i32),
            pltpu.VMEM(queries.shape, bf16),
            pltpu.VMEM(queries.shape, bf16),
            pltpu.VMEM((2, tokens * groups, dh), bf16),
            pltpu.VMEM((2, tokens * groups + 8, dh), f32),
            pltpu.VMEM((pieces, own_blocks, BLK, dh), bf16),
            pltpu.VMEM((pieces, pool_rows, dh), bf16),
            pltpu.VMEM((pieces, pool_blocks, BLK, dh), f32),
            pltpu.VMEM((2, pool_rows, rows), f32),
            pltpu.VMEM((chunks, pool_rows, rows), f32),
            pltpu.VMEM((groups, chunks, slots, rows), f32),
            pltpu.VMEM((groups, chunks, tokens, rows), f32),
            pltpu.VMEM((groups, chunks, pool_rows, rows), bf16),
            pltpu.VMEM((groups, slots, tokens), bf16),
            pltpu.VMEM((groups, n + far_rows, LANES), i32),
            pltpu.VMEM((mates, groups, n + far_rows, LANES), i32),
            pltpu.SMEM((groups, n + far_rows, LANES), i32),
            pltpu.VMEM((pieces, mates, depth, BLK, dh), bf16),
            pltpu.VMEM((pieces, mates, depth, BLK, dh), bf16),
            pltpu.VMEM((pieces, depth, own_blocks, BLK, dh), bf16),
            pltpu.VMEM((pieces, depth, own_blocks, BLK, dh), bf16),
            pltpu.VMEM((pieces, own_blocks, BLK, dh), f32),
            dma((6 + mates,)),
            dma((2, mates)),
            dma((pieces,)),
            dma((pieces, depth)),
            dma((pieces,)),
            dma((pieces, depth)),
            dma((pieces,)),
            dma((pieces,)),
            dma((pieces, mates)),
            dma((pieces, mates, depth)),
            dma((pieces,)),
            dma((pieces,)),
        ] + [pltpu.VMEM((2, chips, own_blocks, BLK, dh), bf16)] * pieces + [pltpu.SMEM((groups, n + far_rows, LANES), i32)] * mates,
        compiler_params=pltpu.CompilerParams(collective_id=0, has_side_effects=True),
    )(
        chosen,
        queries,
        grad_out,
        keys.reshape(tokens * groups, dh),
        values.reshape(tokens * groups, dh),
    )
    held = [pltpu.with_memory_space_constraint(a, pltpu.VMEM) for a in held]
    dq, key_grad, value_grad = store(held)
    return dq, key_grad.reshape(keys.shape), value_grad.reshape(values.shape)


def solution(mesh):
    spec = P(("rep", "ctx"), None, None)
    cols = columns_of(mesh, mesh.shape["ctx"])
    return jax.shard_map(
        functools.partial(local, cols),
        mesh=mesh,
        in_specs=(spec,) * 5,
        out_specs=(spec,) * 3,
        check_vma=False,
    )
```

```python
import functools
import math

import jax
import jax.numpy as jnp
from jax import lax
from jax.experimental import pallas as pl
from jax.experimental.pallas import tpu as pltpu
from jax.sharding import PartitionSpec as P

BLK = 64
NEG = -1e30
BAND = 3
LANES = 128
LOG2E = math.log2(math.e)
NT = (((1,), (1,)), ((), ()))
NN = (((1,), (0,)), ((), ()))


def rows_of(ref, c, chunk_tokens, heads):
    part = ref[c * chunk_tokens : (c + 1) * chunk_tokens, heads, :]
    return part.reshape(part.shape[0] * part.shape[1], part.shape[2])


def bands(total, band=BAND):
    step = BLK * band
    return [(lo, min(lo + step, total)) for lo in range(0, total, step)]


def fold(x, op):
    return op(x.reshape(x.shape[0] // 8, 8, x.shape[1]), axis=0)


def fill_bias(picked, per_group, chunk_tokens, bias_ref, own_bias_ref):
    tokens = picked.shape[1]
    rows = chunk_tokens * per_group
    shift = per_group.bit_length() - 1

    @pl.loop(0, tokens // chunk_tokens)
    def _(c):
        row_tok = c * chunk_tokens + (lax.broadcasted_iota(jnp.int32, (tokens, rows), 1) >> shift)
        tok = lax.broadcasted_iota(jnp.int32, (tokens, rows), 0)
        spread = jnp.where(row_tok == tok, 1.0, 0.0).astype(jnp.bfloat16)
        seen = lax.dot_general(picked, spread, NN, preferred_element_type=jnp.float32)
        bias = (seen - 1.0) * (-NEG)
        bias_ref[c] = bias
        for j in range(tokens // BLK):
            at = slice(j * BLK, (j + 1) * BLK)
            own_bias_ref[c, at] = jnp.where(tok[at] <= row_tok[at], bias[j : j + 1], NEG)


class Weigh:
    def __init__(self, heads, chunk_tokens, bias, own_bias, q_ref, do_ref, keys, s_ref, e_ref, acc_ref):
        self.__dict__.update(locals())
        self.peak, self.inv = {}, {}

    def scores(self, c):
        tokens, _, dh = self.q_ref.shape
        q = rows_of(self.q_ref, c, self.chunk_tokens, self.heads)
        peak = None
        for lo, hi in bands(self.keys.shape[0]):
            s = lax.dot_general(self.keys[lo:hi], q, NT, preferred_element_type=jnp.float32)
            for j in range(lo // BLK, hi // BLK):
                part = s[j * BLK - lo : (j + 1) * BLK - lo]
                if j < tokens // BLK:
                    part = part + self.own_bias[c, j * BLK : (j + 1) * BLK]
                else:
                    part = part + self.bias[c, j : j + 1]
                self.s_ref[c % 2, j * BLK : (j + 1) * BLK] = part
                top = fold(part, jnp.max)
                peak = top if peak is None else jnp.maximum(peak, top)
            yield
        log_scale = LOG2E / math.sqrt(dh)
        self.peak[c] = jnp.max(peak, axis=0, keepdims=True) * log_scale

    def exponents(self, c):
        dh = self.q_ref.shape[2]
        log_scale = LOG2E / math.sqrt(dh)
        total = None
        for lo, hi in bands(self.keys.shape[0]):
            for j in range(lo // BLK, hi // BLK):
                at = slice(j * BLK, (j + 1) * BLK)
                e = jnp.exp2(self.s_ref[c % 2, at] * log_scale - self.peak[c])
                self.e_ref[c, at] = e
                part = fold(e, jnp.sum)
                total = part if total is None else total + part
            yield
        self.inv[c] = 1.0 / jnp.sum(total, axis=0, keepdims=True)

    def products(self, c):
        do = rows_of(self.do_ref, c, self.chunk_tokens, self.heads)
        for lo, hi in bands(self.keys.shape[0]):
            p = self.e_ref[c, lo:hi] * self.inv[c]
            self.e_ref[c, lo:hi] = p
            dv = lax.dot_general(p.astype(jnp.bfloat16), do, NN, preferred_element_type=jnp.float32)
            dv = dv.reshape((hi - lo) // BLK, BLK, dv.shape[1])
            at = slice(lo // BLK, hi // BLK)
            self.acc_ref[at] = dv if c == 0 else self.acc_ref[at] + dv
            yield


class Slope:
    def __init__(self, heads, chunk_tokens, q_ref, do_ref, values, s_ref, e_ref, ds_ref, acc_ref):
        self.__dict__.update(locals())
        self.inner = {}

    def scores(self, c):
        do = rows_of(self.do_ref, c, self.chunk_tokens, self.heads)
        total = None
        for lo, hi in bands(self.values.shape[0], 5):
            dp = lax.dot_general(self.values[lo:hi], do, NT, preferred_element_type=jnp.float32)
            for j in range(lo // BLK, hi // BLK):
                part = dp[j * BLK - lo : (j + 1) * BLK - lo]
                self.s_ref[c % 2, j * BLK : (j + 1) * BLK] = part
                part = fold(part * self.e_ref[c, j * BLK : (j + 1) * BLK], jnp.sum)
                total = part if total is None else total + part
            yield
        self.inner[c] = jnp.sum(total, axis=0, keepdims=True)

    def products(self, c):
        q = rows_of(self.q_ref, c, self.chunk_tokens, self.heads)
        for lo, hi in bands(self.values.shape[0], 5):
            dp = self.s_ref[c % 2, lo:hi]
            ds = (self.e_ref[c, lo:hi] * (dp - self.inner[c])).astype(jnp.bfloat16)
            self.ds_ref[c, lo:hi] = ds
            dk = lax.dot_general(ds, q, NN, preferred_element_type=jnp.float32)
            dk = dk.reshape((hi - lo) // BLK, BLK, dk.shape[1])
            at = slice(lo // BLK, hi // BLK)
            self.acc_ref[at] = dk if c == 0 else self.acc_ref[at] + dk
            yield


def side_by_side(parts):
    parts = list(parts)
    while parts:
        parts = [part for part in parts if next(part, parts) is None]


def pipelined(phases, chunks, between):
    depth = len(phases)
    for t in range(chunks + depth - 1):
        live = [(i, t - i) for i in range(depth) if 0 <= t - i < chunks]
        side_by_side(phases[i](c) for i, c in reversed(live))
        between(t)


def query_grad(c, heads, chunk_tokens, keys_t, ds_ref, dq_ref):
    dh = keys_t.shape[0]
    t0 = pl.multiple_of(c * chunk_tokens, chunk_tokens)
    dqt = lax.dot_general(keys_t, ds_ref[c], NN, preferred_element_type=jnp.float32)
    dq = (dqt * (1.0 / math.sqrt(dh))).T.astype(jnp.bfloat16)
    per_group = heads.stop - heads.start
    dq_ref[pl.ds(t0, chunk_tokens), heads, :] = dq.reshape(chunk_tokens, per_group, dh)


def fill_tables(g, n, me, n_far, own_blocks, sel_ref, picked_ref, tab_ref):
    sel = sel_ref[g]
    tokens = sel.shape[1]
    shift = own_blocks.bit_length() - 1
    owner = sel >> shift
    block = sel & (own_blocks - 1)
    peers = lax.broadcasted_iota(jnp.int32, (n, tokens), 0)
    code = jnp.zeros((n, tokens), jnp.float32)
    for i in range(sel.shape[0]):
        mark = (block[i : i + 1] + 1).astype(jnp.float32)
        code = jnp.maximum(code, jnp.where(owner[i : i + 1] == peers, mark, 0.0))
    code = jnp.broadcast_to(jnp.max(code, axis=1, keepdims=True), (n, LANES))
    peers = lax.broadcasted_iota(jnp.int32, (n, LANES), 0)
    code = jnp.where(peers == me, 0.0, code)
    live = jnp.where(code > 0.0, 1.0, 0.0)
    before = lax.broadcasted_iota(jnp.int32, (n, n), 1) < lax.broadcasted_iota(jnp.int32, (n, n), 0)
    before = jnp.where(before, 1.0, 0.0).astype(jnp.bfloat16)
    slot = lax.dot_general(before, live.astype(jnp.bfloat16), NN, preferred_element_type=jnp.float32)
    far = jnp.maximum(code - 1.0, 0.0)
    lane = lax.broadcasted_iota(jnp.int32, (n, LANES), 1)
    kept = jnp.minimum(slot, float(n_far - 1))
    entry = jnp.where(lane == 0, kept, jnp.where(lane == 1, live, far))
    tab_ref[g, :n, :] = entry.astype(jnp.int32)
    peer = peers.astype(jnp.float32)
    now = me * own_blocks + (lax.broadcasted_iota(jnp.int32, (1, tokens), 1) >> BLK.bit_length() - 1)
    slots = picked_ref.shape[1]
    row = lax.broadcasted_iota(jnp.int32, (slots, tokens), 0)
    far_rows = tab_ref.shape[1] - n
    far_row = lax.broadcasted_iota(jnp.int32, (far_rows, LANES), 0)
    far_lane = lax.broadcasted_iota(jnp.int32, (far_rows, LANES), 1)
    far_entry = jnp.zeros((far_rows, LANES), jnp.float32)
    picked = jnp.zeros((slots, tokens), jnp.float32)
    for i in range(own_blocks + n_far):
        if i < own_blocks:
            ids = jnp.full((1, tokens), me * own_blocks + i, jnp.int32)
        else:
            hit = (live > 0.0) & (slot == float(i - own_blocks))
            who = jnp.max(jnp.where(hit, peer, -1.0), axis=0, keepdims=True)
            which = jnp.max(jnp.where(hit, far, 0.0), axis=0, keepdims=True)
            ids = jnp.max(who * own_blocks + which, axis=1, keepdims=True).astype(jnp.int32)
            ids = jnp.broadcast_to(ids, (1, tokens))
            here = jnp.where(far_lane == 0, jnp.maximum(who, 0.0), which)
            far_entry = jnp.where(far_row == i - own_blocks, here, far_entry)
        seen = jnp.max(jnp.where(sel == ids, 1.0, 0.0), axis=0, keepdims=True)
        seen = jnp.where(ids <= now, seen, 0.0)
        picked = jnp.where(row == i, seen, picked)
    tab_ref[g, n:, :] = far_entry.astype(jnp.int32)
    picked_ref[g] = picked.astype(jnp.bfloat16)


def fused_kernel(
    n, cols, n_far, chunk_tokens, groups,
    sel_hbm, q_hbm, do_hbm, k_hbm, v_hbm, dq_ref, key_out, value_out,
    sel_ref, q_ref, do_ref, raw_ref, mix_ref, own, pool, acc, s_ref, e_ref, bias_ref, own_bias_ref, ds_ref,
    picked_ref, tab_ref, mate_tab_ref, tab, mate_tab, box, box_in, z_box, z_in, total_ref,
    in_sem, done, tab_sem, zr, yr, sr, box_recv, rz_recv, *banks,
):
    gaths = list(banks)
    depth = n // (2 * cols)
    chips = n // 2
    me = lax.axis_index("ctx")
    core = lax.rem(me, 2)
    chip = me // 2
    y = lax.rem(chip, cols)
    z = chip // cols
    sib = 2 * chip + 1 - core
    other_y = cols - 1 - y
    y_peer = 2 * (z * cols + other_y) + core
    own_blocks = own.shape[1]
    own_rows = own_blocks * BLK
    dh = own.shape[3]
    per_group = q_ref.shape[1] // groups
    chunks = q_ref.shape[0] // chunk_tokens
    scaling = 1.0 / math.sqrt(dh)
    pieces = 2 * groups
    near_max = depth - 1

    def device(zz, yy, cc):
        return 2 * (zz * cols + yy) + cc

    def near(k):
        room = jnp.minimum(z, depth - 1 - z)
        step = jnp.where(lax.rem(k, 2) == 1, -((k + 1) // 2), k // 2)
        side = jnp.where(z < depth - 1 - z, k - room, room - k)
        return z + jnp.where(k <= 2 * room, step, side)

    def remote(src, dst, send, recv, peer):
        return pltpu.make_async_remote_copy(
            src_ref=src,
            dst_ref=dst,
            send_sem=send,
            recv_sem=recv,
            device_id={"ctx": peer},
            device_id_type=pl.DeviceIdType.MESH,
        )

    def turn(k):
        return jnp.where(core == 0, depth - k, jnp.where(k == 1, 1, depth + 1 - k))

    def z_send(p, src, from_z, to_z):
        dst = gaths[p].at[core, from_z * cols + y]
        return remote(src, dst, done, zr.at[p, from_z], device(to_z, y, core))

    def z_wait(p, from_z):
        spot = gaths[p].at[core, from_z * cols + y]
        remote(spot, spot, done, zr.at[p, from_z], y_peer if cols > 1 else sib).wait_recv()

    def y_send(p, src, from_z):
        dst = gaths[p].at[core, from_z * cols + y]
        return remote(src, dst, done, yr.at[p, from_z], y_peer)

    def y_wait(p, from_z):
        spot = gaths[p].at[core, from_z * cols + other_y]
        remote(spot, spot, done, yr.at[p, from_z], y_peer).wait_recv()

    def sib_send(p, src, q):
        return remote(src, gaths[p].at[core, q], done, sr.at[p], sib)

    def gather_start(p):
        if cols > 1:
            y_send(p, own.at[p], z).start()

        @pl.loop(1, depth)
        def _(k):
            z_send(p, own.at[p], z, near(turn(k))).start()

        sib_send(p, own.at[p], chip).start()

    def span(i):
        return 1 + i * near_max // 3, 1 + (i + 1) * near_max // 3

    pair = z + 1 - 2 * lax.rem(z, 2)

    def each_at(d, visit):
        for side in (-1, 1):
            from_z = z + side * d

            @pl.when((from_z >= 0) & (from_z < depth))
            def _():
                visit(from_z)

    def z_step(p, i):
        lo, hi = span(i)

        def visit(from_z):
            q = from_z * cols + y
            spot = gaths[p].at[core, q]
            z_wait(p, from_z)

            if cols > 1:
                @pl.when((core == 1) | (from_z != pair) | (pair >= depth))
                def _():
                    y_send(p, spot, from_z).start()

            sib_send(p, spot, q).start()

        @pl.loop(lo, hi)
        def _(d):
            each_at(d, visit)

    def y_step(p, i):
        if cols == 1:
            return

        def visit(from_z):
            q = from_z * cols + other_y
            spot = gaths[p].at[core, q]
            y_wait(p, from_z)
            if i == 0:
                @pl.when((core == 0) & (pair < depth))
                def _():
                    remote(spot, spot, done, yr.at[p, z], device(pair, y, core)).start()

            sib_send(p, spot, q).start()

        if i == 0:
            visit(z)
        else:
            lo, hi = span(i - 1)

            @pl.loop(lo, hi)
            def _(d):
                each_at(d, visit)

    def gather_end(p):
        spot = gaths[p].at[1 - core]
        remote(spot, spot, done, sr.at[p], sib).wait_recv()

    def gather_drain(p):
        spot = gaths[p].at[core]
        remote(spot, spot, done, sr.at[p], sib).wait_send()
        part = gaths[p].at[core, pl.ds(0, depth - 1)]
        remote(part, part, done, zr.at[p, z], sib).wait_send()
        if cols > 1:
            part = gaths[p].at[core, pl.ds(0, depth)]
            remote(part, part, done, yr.at[p, z], y_peer).wait_send()

    def fill_pool(p):
        g = p // 2
        pool[p, :own_rows, :] = own[p].reshape(own_rows, dh)
        for s in range(n_far):
            owner = jnp.clip(tab[g, n + s, 0], 0, n - 1)
            block = jnp.clip(tab[g, n + s, 1], 0, own_blocks - 1)
            lo = own_rows + s * BLK
            pool[p, lo : lo + BLK, :] = gaths[p][owner & 1, owner >> 1, block]

    mates = [(y, 1 - core)] + ([(other_y, core), (other_y, 1 - core)] if cols > 1 else [])

    def mate_copy(p, m, zz):
        return remote(
            box.at[p, zz, m], box_in.at[p, zz, m], done, box_recv.at[p, zz],
            device(z, *mates[m]),
        )

    def z_copy(p, to_z):
        return remote(
            z_box.at[p, to_z], z_in.at[p, z], done, rz_recv.at[p], device(to_z, y, core)
        )

    def factor(p):
        return scaling if p % 2 == 0 else 1.0

    def far_part(p, dest):
        return acc[p, own_blocks + jnp.clip(tab[p // 2, dest, 0], 0, n_far - 1)]

    def far_first(k):
        return jnp.where(k == depth, z, near(jnp.maximum(depth - k, 1)))

    def return_start(p):
        g = p // 2

        @pl.loop(1, depth + 1)
        def _(k):
            zz = far_first(k)
            for m, (yy, cc) in enumerate(mates):
                dest = device(zz, yy, cc)
                keep = tab[g, dest, 1].astype(jnp.float32) * factor(p)
                box[p, zz, m] = (far_part(p, dest) * keep).astype(jnp.bfloat16)
            for m in range(len(mates)):
                mate_copy(p, m, zz).start()

    def merged(p, zz):
        g = p // 2
        dest = device(zz, y, core)
        spot = box_in.at[p, zz]
        remote(spot, spot, done, box_recv.at[p, zz], sib).wait_recv()
        parts = [far_part(p, dest) * (tab[g, dest, 1].astype(jnp.float32) * factor(p))]
        tables = [tab] + [mate_tab.at[m] for m in range(len(mates))]
        for m in range(len(mates)):
            parts.append(box_in[p, zz, m].astype(jnp.float32))
        for b in range(own_blocks):
            total = None
            for table, part in zip(tables, parts):
                share = part * jnp.where(table[g, dest, 2] == b, 1.0, 0.0)
                total = share if total is None else total + share
            yield b, total

    def return_column(p, i):
        lo, hi = span(i)

        @pl.loop(lo, hi)
        def _(k):
            to_z = far_first(k)
            for b, part in merged(p, to_z):
                z_box[p, to_z, b] = part.astype(jnp.bfloat16)
            z_copy(p, to_z).start()

    def return_own(p):
        for b, part in merged(p, z):
            total_ref[p, b] = part + acc[p, b] * factor(p)

    def return_end(p):
        part = z_in.at[p, pl.ds(0, depth - 1)]
        remote(part, part, done, rz_recv.at[p], sib).wait_recv()

        @pl.loop(1, depth)
        def _(k):
            from_z = near(k)
            total_ref[p] += z_in[p, from_z].astype(jnp.float32)

        whole = total_ref[p].reshape(own_rows, dh)
        mix_ref[p % 2, pl.ds(p // 2, own_rows, stride=groups), :] = whole

    def return_drain(p):
        part = box.at[p]
        remote(part, part, done, box_recv.at[p, 0], sib).wait_send()
        part = z_box.at[p, pl.ds(0, depth - 1)]
        remote(part, part, done, rz_recv.at[p], sib).wait_send()

    barrier = pltpu.get_barrier_semaphore()

    def greet(peer):
        pl.semaphore_signal(
            barrier, inc=1, device_id={"ctx": peer}, device_id_type=pl.DeviceIdType.MESH
        )

    @pl.loop(1, depth)
    def _(k):
        greet(device(near(k), y, core))

    for yy, cc in mates:
        greet(device(z, yy, cc))
    kv_loads = [
        pltpu.make_async_copy(k_hbm, raw_ref.at[0], in_sem.at[0]),
        pltpu.make_async_copy(v_hbm, raw_ref.at[1], in_sem.at[1]),
    ]
    sel_load = pltpu.make_async_copy(sel_hbm, sel_ref, in_sem.at[2])
    rest = [
        pltpu.make_async_copy(q_hbm, q_ref, in_sem.at[3]),
        pltpu.make_async_copy(do_hbm, do_ref, in_sem.at[4]),
    ]
    for load in kv_loads + [sel_load] + rest:
        load.start()
    for kv in range(2):
        kv_loads[kv].wait()
        mix_ref[kv, : own_rows * groups] = raw_ref[kv].astype(jnp.float32)
        for g in range(groups):
            rows = mix_ref[kv, pl.ds(g, own_rows, stride=groups), :].astype(jnp.bfloat16)
            own[2 * g + kv] = rows.reshape(own_blocks, BLK, dh)
    pl.semaphore_wait(barrier, depth - 1 + len(mates))
    gather_start(0)
    sel_load.wait()
    for g in range(groups):
        fill_tables(g, n, me, n_far, own_blocks, sel_ref, picked_ref, tab_ref)
    to_scalars = pltpu.make_async_copy(tab_ref, tab, in_sem.at[2])
    to_scalars.start()
    to_mates = [
        remote(
            tab_ref, mate_tab_ref.at[m], done, tab_sem, device(z, yy, cc)
        )
        for m, (yy, cc) in enumerate(mates)
    ]
    for copy in to_mates:
        copy.start()
    gather_start(1)
    for g in range(groups):
        fill_bias(picked_ref[g], per_group, chunk_tokens, bias_ref.at[g], own_bias_ref.at[g])
    to_scalars.wait()
    for load in rest:
        load.wait()

    def run(steps):
        for name, *args in steps:
            {
                "z": z_step, "y": y_step, "end": gather_end, "pool": fill_pool,
                "start": return_start, "column": return_column,
                "own": return_own, "done": return_end,
            }[name](*args)

    K0, V0, K1, V1 = range(4) if groups == 2 else (0, 1, None, None)

    def stage(body, plan):
        @pl.loop(0, chunks)
        def _(c):
            body(c)
            for i, steps in enumerate(plan):
                @pl.when(c == min(i, chunks - 1))
                def _():
                    run(steps)

    def heads(g):
        return slice(g * per_group, (g + 1) * per_group)

    def between(plan):
        return lambda t: run(plan[t] if t < len(plan) else [])

    def weigh_stage(g, plan):
        work = Weigh(
            heads(g), chunk_tokens, bias_ref.at[g], own_bias_ref.at[g], q_ref, do_ref,
            pool.at[2 * g], s_ref, e_ref, acc.at[2 * g + 1],
        )
        pipelined([work.scores, work.exponents, work.products], chunks, between(plan))

    def slope_stage(g, plan):
        work = Slope(
            heads(g), chunk_tokens, q_ref, do_ref, pool.at[2 * g + 1], s_ref, e_ref,
            ds_ref.at[g], acc.at[2 * g],
        )
        pipelined([work.scores, work.products], chunks, between(plan))

    def query_stage(g, plan):
        keys_t = pool[2 * g].T
        stage(lambda c: query_grad(c, heads(g), chunk_tokens, keys_t, ds_ref.at[g], dq_ref), plan)

    for p in range(2, pieces):
        gather_start(p)
    run([("y", K0, 0), ("z", K0, 0), ("z", K0, 1), ("z", K0, 2), ("y", V0, 0)])
    remote(mate_tab_ref, mate_tab_ref, done, tab_sem, sib).wait_recv()
    back = pltpu.make_async_copy(mate_tab_ref, mate_tab, in_sem.at[3])
    back.start()
    run([("y", K1, 0), ("y", V1, 0), ("z", V0, 0), ("z", V0, 1), ("z", V0, 2), ("y", K0, 1),
         ("y", K0, 2), ("y", K0, 3), ("end", K0), ("pool", K0)])
    back.wait()
    weigh_stage(0, [
        [],
        [("z", K1, 0)],
        [("y", V0, 1)],
        [("z", K1, 1)],
        [("y", V0, 2), ("z", K1, 2)],
        [("y", V0, 3), ("z", V1, 0)],
    ])
    run([("z", V1, 1), ("end", V0), ("pool", V0)])
    slope_stage(0, [
        [("z", V1, 2), ("y", K1, 1)],
        [],
        [("start", V0), ("y", K1, 2)],
        [("y", K1, 3)],
    ])
    run([("start", K0), ("y", V1, 1), ("end", K1), ("pool", K1)])
    weigh_stage(1, [
        [],
        [("y", V1, 2)],
        [],
        [("y", V1, 3)],
        [("column", V0, 0)],
        [("column", V0, 1)],
    ])
    run([("start", V1), ("end", V1), ("pool", V1)])
    slope_stage(1, [
        [("column", V0, 2)],
        [("column", K0, 0)],
        [("column", K0, 1)],
        [("column", K0, 2)],
    ])
    run([("start", K1), ("own", V0), ("own", K0)])
    query_stage(0, [
        [("column", V1, 0)],
        [("column", V1, 1)],
        [("column", V1, 2)],
        [("done", V0)],
    ])
    query_stage(1, [
        [],
        [("own", V1), ("column", K1, 0), ("column", K1, 1), ("column", K1, 2)],
        [("own", K1)],
        [("done", K0), ("done", V1)],
    ])
    run([("done", K1)])
    remote(mate_tab_ref, mate_tab_ref, done, tab_sem, sib).wait_send()
    for p in range(pieces):
        gather_drain(p)
        return_drain(p)
    key_out[...] = mix_ref[0, : own_rows * groups].astype(jnp.bfloat16)
    value_out[...] = mix_ref[1, : own_rows * groups].astype(jnp.bfloat16)


def store_kernel(*refs):
    count = (len(refs) - 1) // 2
    sem = refs[-1]
    copies = [
        pltpu.make_async_copy(refs[i], refs[count + i], sem.at[i]) for i in range(count)
    ]
    for copy in copies:
        copy.start()
    for copy in copies:
        copy.wait()


def store(arrays):
    return pl.pallas_call(
        store_kernel,
        out_shape=tuple(jax.ShapeDtypeStruct(a.shape, a.dtype) for a in arrays),
        in_specs=[pl.BlockSpec(memory_space=pltpu.VMEM)] * len(arrays),
        out_specs=(pl.BlockSpec(memory_space=pl.ANY),) * len(arrays),
        scratch_shapes=[pltpu.SemaphoreType.DMA((len(arrays),))],
    )(*arrays)


def columns_of(mesh, n):
    spots = [getattr(d, "coords", None) for d in mesh.devices.reshape(-1, n)[0]]
    if None in spots or n % 2:
        return 1
    cols = sum(spot[2] == spots[0][2] for spot in spots) // 2
    return 2 if cols == 2 and n % 4 == 0 else 1


def local(cols, queries, keys, values, grad_out, selected):
    tokens, head_count, dh = queries.shape
    groups = keys.shape[1]
    own_blocks = tokens // BLK
    n = lax.axis_size("ctx")
    depth = n // (2 * cols)
    chips = n // 2
    pieces = 2 * groups
    fetched = min(n - 2, max(selected.shape[2] - own_blocks, 4)) + 1
    slots = -(-(own_blocks + fetched) // 16) * 16
    far_rows = -(-fetched // 8) * 8
    pool_blocks = own_blocks + fetched
    pool_rows = pool_blocks * BLK
    chunk_tokens = min(tokens, 32)
    chunks = tokens // chunk_tokens
    rows = chunk_tokens * head_count // groups
    chosen = selected.transpose(1, 2, 0)
    mates = 3 if cols > 1 else 1
    any_spec = pl.BlockSpec(memory_space=pl.ANY)
    vmem = pl.BlockSpec(memory_space=pltpu.VMEM)
    dma = pltpu.SemaphoreType.DMA
    bf16, f32, i32 = jnp.bfloat16, jnp.float32, jnp.int32
    held = pl.pallas_call(
        functools.partial(fused_kernel, n, cols, fetched, chunk_tokens, groups),
        out_shape=(
            pltpu.VMEM(queries.shape, bf16),
            pltpu.VMEM((tokens * groups, dh), bf16),
            pltpu.VMEM((tokens * groups, dh), bf16),
        ),
        in_specs=[any_spec] * 5,
        out_specs=(vmem, vmem, vmem),
        scratch_shapes=[
            pltpu.VMEM(chosen.shape, i32),
            pltpu.VMEM(queries.shape, bf16),
            pltpu.VMEM(queries.shape, bf16),
            pltpu.VMEM((2, tokens * groups, dh), bf16),
            pltpu.VMEM((2, tokens * groups + 8, dh), f32),
            pltpu.VMEM((pieces, own_blocks, BLK, dh), bf16),
            pltpu.VMEM((pieces, pool_rows, dh), bf16),
            pltpu.VMEM((pieces, pool_blocks, BLK, dh), f32),
            pltpu.VMEM((2, pool_rows, rows), f32),
            pltpu.VMEM((chunks, pool_rows, rows), f32),
            pltpu.VMEM((groups, chunks, slots, rows), f32),
            pltpu.VMEM((groups, chunks, tokens, rows), f32),
            pltpu.VMEM((groups, chunks, pool_rows, rows), bf16),
            pltpu.VMEM((groups, slots, tokens), bf16),
            pltpu.VMEM((groups, n + far_rows, LANES), i32),
            pltpu.VMEM((mates, groups, n + far_rows, LANES), i32),
            pltpu.SMEM((groups, n + far_rows, LANES), i32),
            pltpu.SMEM((mates, groups, n + far_rows, LANES), i32),
            pltpu.VMEM((pieces, depth, mates, BLK, dh), bf16),
            pltpu.VMEM((pieces, depth, mates, BLK, dh), bf16),
            pltpu.VMEM((pieces, depth, own_blocks, BLK, dh), bf16),
            pltpu.VMEM((pieces, depth, own_blocks, BLK, dh), bf16),
            pltpu.VMEM((pieces, own_blocks, BLK, dh), f32),
            dma((5,)),
            dma,
            dma,
            dma((pieces, depth)),
            dma((pieces, depth)),
            dma((pieces,)),
            dma((pieces, depth)),
            dma((pieces,)),
        ] + [pltpu.VMEM((2, chips, own_blocks, BLK, dh), bf16)] * pieces,
        compiler_params=pltpu.CompilerParams(collective_id=0, has_side_effects=True),
    )(
        chosen,
        queries,
        grad_out,
        keys.reshape(tokens * groups, dh),
        values.reshape(tokens * groups, dh),
    )
    held = [pltpu.with_memory_space_constraint(a, pltpu.VMEM) for a in held]
    dq, key_grad, value_grad = store(held)
    return dq, key_grad.reshape(keys.shape), value_grad.reshape(values.shape)


def solution(mesh):
    spec = P(("rep", "ctx"), None, None)
    cols = columns_of(mesh, mesh.shape["ctx"])
    return jax.shard_map(
        functools.partial(local, cols),
        mesh=mesh,
        in_specs=(spec,) * 5,
        out_specs=(spec,) * 3,
        check_vma=False,
    )
```

```python
import functools
import math

import jax
import jax.numpy as jnp
from jax import lax
from jax.experimental import pallas as pl
from jax.experimental.pallas import tpu as pltpu
from jax.sharding import PartitionSpec as P

BLK = 64
NEG = -1e30
BAND = 3
LANES = 128
LOG2E = math.log2(math.e)
NT = (((1,), (1,)), ((), ()))
NN = (((1,), (0,)), ((), ()))


def rows_of(ref, c, chunk_tokens, heads):
    part = ref[c * chunk_tokens : (c + 1) * chunk_tokens, heads, :]
    return part.reshape(part.shape[0] * part.shape[1], part.shape[2])


def bands(total, start=0):
    step = BLK * BAND
    return [(lo, min(lo + step, total)) for lo in range(start, total, step)]


def fold(x, op):
    return op(x.reshape(x.shape[0] // 8, 8, x.shape[1]), axis=0)


def fill_own(g, per_group, chunk_tokens, picked, q_ref, do_ref, own, bias_ref, score_ref, peak_ref, slope_ref):
    tokens, dh = picked.shape[1], own.shape[3]
    rows = chunk_tokens * per_group
    shift = per_group.bit_length() - 1
    heads = slice(g * per_group, (g + 1) * per_group)

    @pl.loop(0, tokens // chunk_tokens)
    def _(c):
        t0 = pl.multiple_of(c * chunk_tokens, chunk_tokens)
        q = q_ref[pl.ds(t0, chunk_tokens), heads, :].reshape(rows, dh)
        do = do_ref[pl.ds(t0, chunk_tokens), heads, :].reshape(rows, dh)
        row_tok = t0 + (lax.broadcasted_iota(jnp.int32, (tokens, rows), 1) >> shift)
        tok = lax.broadcasted_iota(jnp.int32, (tokens, rows), 0)
        spread = jnp.where(row_tok == tok, 1.0, 0.0).astype(jnp.bfloat16)
        seen = lax.dot_general(picked, spread, NN, preferred_element_type=jnp.float32)
        bias = (seen - 1.0) * (-NEG)
        bias_ref[c] = bias
        keys, values = own[2 * g].reshape(tokens, dh), own[2 * g + 1].reshape(tokens, dh)
        s = lax.dot_general(keys, q, NT, preferred_element_type=jnp.float32)
        slope_ref[c] = lax.dot_general(values, do, NT, preferred_element_type=jnp.float32)
        peak = None
        for j in range(tokens // BLK):
            at = slice(j * BLK, (j + 1) * BLK)
            part = jnp.where(tok[at] <= row_tok[at], s[at] + bias[j : j + 1], NEG)
            score_ref[c, at] = part
            top = fold(part, jnp.max)
            peak = top if peak is None else jnp.maximum(peak, top)
        peak_ref[c] = peak


class Weigh:
    def __init__(self, heads, chunk_tokens, bias, own_score, own_peak, q_ref, do_ref, keys, s_ref, e_ref, acc_ref):
        self.__dict__.update(locals())
        self.peak, self.inv = {}, {}

    def scores(self, c):
        tokens, _, dh = self.q_ref.shape
        q = rows_of(self.q_ref, c, self.chunk_tokens, self.heads)
        peak = self.own_peak[c]
        for lo, hi in bands(self.keys.shape[0], tokens):
            s = lax.dot_general(self.keys[lo:hi], q, NT, preferred_element_type=jnp.float32)
            for j in range(lo // BLK, hi // BLK):
                part = s[j * BLK - lo : (j + 1) * BLK - lo]
                part = part + self.bias[c, j : j + 1]
                self.s_ref[c % 2, j * BLK : (j + 1) * BLK] = part
                top = fold(part, jnp.max)
                peak = jnp.maximum(peak, top)
            yield
        log_scale = LOG2E / math.sqrt(dh)
        self.peak[c] = jnp.max(peak, axis=0, keepdims=True) * log_scale

    def exponents(self, c):
        dh = self.q_ref.shape[2]
        log_scale = LOG2E / math.sqrt(dh)
        total = None
        for lo, hi in bands(self.keys.shape[0]):
            for j in range(lo // BLK, hi // BLK):
                at = slice(j * BLK, (j + 1) * BLK)
                far = j >= self.own_score.shape[1] // BLK
                s = self.s_ref[c % 2, at] if far else self.own_score[c, at]
                e = jnp.exp2(s * log_scale - self.peak[c])
                self.e_ref[c, at] = e
                part = fold(e, jnp.sum)
                total = part if total is None else total + part
            yield
        self.inv[c] = 1.0 / jnp.sum(total, axis=0, keepdims=True)

    def products(self, c):
        do = rows_of(self.do_ref, c, self.chunk_tokens, self.heads)
        for lo, hi in bands(self.keys.shape[0]):
            p = self.e_ref[c, lo:hi] * self.inv[c]
            self.e_ref[c, lo:hi] = p
            dv = lax.dot_general(p.astype(jnp.bfloat16), do, NN, preferred_element_type=jnp.float32)
            dv = dv.reshape((hi - lo) // BLK, BLK, dv.shape[1])
            at = slice(lo // BLK, hi // BLK)
            self.acc_ref[at] = dv if c == 0 else self.acc_ref[at] + dv
            yield


class Slope:
    def __init__(self, heads, chunk_tokens, own_slope, q_ref, do_ref, values, s_ref, e_ref, ds_ref, acc_ref):
        self.__dict__.update(locals())
        self.inner = {}

    def scores(self, c):
        do = rows_of(self.do_ref, c, self.chunk_tokens, self.heads)
        own_rows = self.own_slope.shape[1]
        total = fold(self.own_slope[c] * self.e_ref[c, :own_rows], jnp.sum)
        for lo, hi in bands(self.values.shape[0], own_rows):
            dp = lax.dot_general(self.values[lo:hi], do, NT, preferred_element_type=jnp.float32)
            for j in range(lo // BLK, hi // BLK):
                part = dp[j * BLK - lo : (j + 1) * BLK - lo]
                self.s_ref[c % 2, j * BLK : (j + 1) * BLK] = part
                part = fold(part * self.e_ref[c, j * BLK : (j + 1) * BLK], jnp.sum)
                total = total + part
            yield
        self.inner[c] = jnp.sum(total, axis=0, keepdims=True)

    def products(self, c):
        q = rows_of(self.q_ref, c, self.chunk_tokens, self.heads)
        own_rows = self.own_slope.shape[1]
        for lo, hi in [(0, own_rows)] + bands(self.values.shape[0], own_rows):
            dp = self.s_ref[c % 2, lo:hi] if lo >= own_rows else self.own_slope[c]
            ds = (self.e_ref[c, lo:hi] * (dp - self.inner[c])).astype(jnp.bfloat16)
            self.ds_ref[c, lo:hi] = ds
            dk = lax.dot_general(ds, q, NN, preferred_element_type=jnp.float32)
            dk = dk.reshape((hi - lo) // BLK, BLK, dk.shape[1])
            at = slice(lo // BLK, hi // BLK)
            self.acc_ref[at] = dk if c == 0 else self.acc_ref[at] + dk
            yield


def side_by_side(parts):
    parts = list(parts)
    while parts:
        parts = [part for part in parts if next(part, parts) is None]


def pipelined(phases, chunks, between):
    depth = len(phases)
    for t in range(chunks + depth - 1):
        live = [(i, t - i) for i in range(depth) if 0 <= t - i < chunks]
        side_by_side(phases[i](c) for i, c in reversed(live))
        between(t)


def query_grad(c, heads, chunk_tokens, keys_t, ds_ref, dq_ref):
    dh = keys_t.shape[0]
    t0 = pl.multiple_of(c * chunk_tokens, chunk_tokens)
    dqt = lax.dot_general(keys_t, ds_ref[c], NN, preferred_element_type=jnp.float32)
    dq = (dqt * (1.0 / math.sqrt(dh))).T.astype(jnp.bfloat16)
    per_group = heads.stop - heads.start
    dq_ref[pl.ds(t0, chunk_tokens), heads, :] = dq.reshape(chunk_tokens, per_group, dh)


def fill_tables(g, n, me, n_far, own_blocks, sel_ref, picked_ref, tab_ref):
    sel = sel_ref[g]
    tokens = sel.shape[1]
    shift = own_blocks.bit_length() - 1
    owner = sel >> shift
    block = sel & (own_blocks - 1)
    peers = lax.broadcasted_iota(jnp.int32, (n, tokens), 0)
    code = jnp.zeros((n, tokens), jnp.float32)
    for i in range(sel.shape[0]):
        mark = (block[i : i + 1] + 1).astype(jnp.float32)
        code = jnp.maximum(code, jnp.where(owner[i : i + 1] == peers, mark, 0.0))
    code = jnp.broadcast_to(jnp.max(code, axis=1, keepdims=True), (n, LANES))
    peers = lax.broadcasted_iota(jnp.int32, (n, LANES), 0)
    code = jnp.where(peers == me, 0.0, code)
    live = jnp.where(code > 0.0, 1.0, 0.0)
    before = lax.broadcasted_iota(jnp.int32, (n, n), 1) < lax.broadcasted_iota(jnp.int32, (n, n), 0)
    before = jnp.where(before, 1.0, 0.0).astype(jnp.bfloat16)
    slot = lax.dot_general(before, live.astype(jnp.bfloat16), NN, preferred_element_type=jnp.float32)
    far = jnp.maximum(code - 1.0, 0.0)
    lane = lax.broadcasted_iota(jnp.int32, (n, LANES), 1)
    kept = jnp.minimum(slot, float(n_far - 1))
    entry = jnp.where(lane == 0, kept, jnp.where(lane == 1, live, far))
    tab_ref[g, :n, :] = entry.astype(jnp.int32)
    peer = peers.astype(jnp.float32)
    now = me * own_blocks + (lax.broadcasted_iota(jnp.int32, (1, tokens), 1) >> BLK.bit_length() - 1)
    slots = picked_ref.shape[1]
    row = lax.broadcasted_iota(jnp.int32, (slots, tokens), 0)
    far_rows = tab_ref.shape[1] - n
    far_row = lax.broadcasted_iota(jnp.int32, (far_rows, LANES), 0)
    far_lane = lax.broadcasted_iota(jnp.int32, (far_rows, LANES), 1)
    far_entry = jnp.zeros((far_rows, LANES), jnp.float32)
    picked = jnp.zeros((slots, tokens), jnp.float32)
    for i in range(own_blocks + n_far):
        if i < own_blocks:
            ids = jnp.full((1, tokens), me * own_blocks + i, jnp.int32)
        else:
            hit = (live > 0.0) & (slot == float(i - own_blocks))
            who = jnp.max(jnp.where(hit, peer, -1.0), axis=0, keepdims=True)
            which = jnp.max(jnp.where(hit, far, 0.0), axis=0, keepdims=True)
            ids = jnp.max(who * own_blocks + which, axis=1, keepdims=True).astype(jnp.int32)
            ids = jnp.broadcast_to(ids, (1, tokens))
            here = jnp.where(far_lane == 0, jnp.maximum(who, 0.0), which)
            far_entry = jnp.where(far_row == i - own_blocks, here, far_entry)
        seen = jnp.max(jnp.where(sel == ids, 1.0, 0.0), axis=0, keepdims=True)
        seen = jnp.where(ids <= now, seen, 0.0)
        picked = jnp.where(row == i, seen, picked)
    tab_ref[g, n:, :] = far_entry.astype(jnp.int32)
    picked_ref[g] = picked.astype(jnp.bfloat16)


def fused_kernel(
    n, cols, n_far, chunk_tokens, groups,
    sel_hbm, q_hbm, do_hbm, k_hbm, v_hbm, dq_ref, key_out, value_out,
    sel_ref, q_ref, do_ref, raw_ref, mix_ref, own, pool, acc, s_ref, e_ref, bias_ref, own_score_ref, own_peak_ref, own_slope_ref, ds_ref,
    picked_ref, tab_ref, mate_tab_ref, tab, mate_tab, box, box_in, z_box, z_in, total_ref,
    in_sem, done, tab_sem, zr, yr, sr, box_recv, rz_recv, *banks,
):
    gaths = list(banks)
    depth = n // (2 * cols)
    chips = n // 2
    me = lax.axis_index("ctx")
    core = lax.rem(me, 2)
    chip = me // 2
    y = lax.rem(chip, cols)
    z = chip // cols
    sib = 2 * chip + 1 - core
    other_y = cols - 1 - y
    y_peer = 2 * (z * cols + other_y) + core
    own_blocks = own.shape[1]
    own_rows = own_blocks * BLK
    dh = own.shape[3]
    per_group = q_ref.shape[1] // groups
    chunks = q_ref.shape[0] // chunk_tokens
    scaling = 1.0 / math.sqrt(dh)
    pieces = 2 * groups
    near_max = depth - 1

    def device(zz, yy, cc):
        return 2 * (zz * cols + yy) + cc

    def near(k):
        room = jnp.minimum(z, depth - 1 - z)
        step = jnp.where(lax.rem(k, 2) == 1, -((k + 1) // 2), k // 2)
        side = jnp.where(z < depth - 1 - z, k - room, room - k)
        return z + jnp.where(k <= 2 * room, step, side)

    def remote(src, dst, send, recv, peer):
        return pltpu.make_async_remote_copy(
            src_ref=src,
            dst_ref=dst,
            send_sem=send,
            recv_sem=recv,
            device_id={"ctx": peer},
            device_id_type=pl.DeviceIdType.MESH,
        )

    def turn(k):
        return jnp.where(core == 0, depth - k, jnp.where(k == 1, 1, depth + 1 - k))

    def z_send(p, src, from_z, to_z):
        dst = gaths[p].at[core, from_z * cols + y]
        return remote(src, dst, done, zr.at[p, from_z], device(to_z, y, core))

    def z_wait(p, from_z):
        spot = gaths[p].at[core, from_z * cols + y]
        remote(spot, spot, done, zr.at[p, from_z], y_peer if cols > 1 else sib).wait_recv()

    def y_send(p, src, from_z):
        dst = gaths[p].at[core, from_z * cols + y]
        return remote(src, dst, done, yr.at[p, from_z], y_peer)

    def y_wait(p, from_z):
        spot = gaths[p].at[core, from_z * cols + other_y]
        remote(spot, spot, done, yr.at[p, from_z], y_peer).wait_recv()

    def sib_send(p, src, q):
        return remote(src, gaths[p].at[core, q], done, sr.at[p], sib)

    def gather_start(p):
        if cols > 1:
            y_send(p, own.at[p], z).start()

        @pl.loop(1, depth)
        def _(k):
            z_send(p, own.at[p], z, near(turn(k))).start()

        sib_send(p, own.at[p], chip).start()

    def span(i):
        return 1 + i * near_max // 3, 1 + (i + 1) * near_max // 3

    pair = z + 1 - 2 * lax.rem(z, 2)

    def each_at(d, visit):
        for side in (-1, 1):
            from_z = z + side * d

            @pl.when((from_z >= 0) & (from_z < depth))
            def _():
                visit(from_z)

    def z_step(p, i):
        lo, hi = span(i)

        def visit(from_z):
            q = from_z * cols + y
            spot = gaths[p].at[core, q]
            z_wait(p, from_z)

            if cols > 1:
                @pl.when((core == 1) | (from_z != pair) | (pair >= depth))
                def _():
                    y_send(p, spot, from_z).start()

            sib_send(p, spot, q).start()

        @pl.loop(lo, hi)
        def _(d):
            each_at(d, visit)

    def y_step(p, i):
        if cols == 1:
            return

        def visit(from_z):
            q = from_z * cols + other_y
            spot = gaths[p].at[core, q]
            y_wait(p, from_z)
            if i == 0:
                @pl.when((core == 0) & (pair < depth))
                def _():
                    remote(spot, spot, done, yr.at[p, z], device(pair, y, core)).start()

            sib_send(p, spot, q).start()

        if i == 0:
            visit(z)
        else:
            lo, hi = span(i - 1)

            @pl.loop(lo, hi)
            def _(d):
                each_at(d, visit)

    def gather_end(p):
        spot = gaths[p].at[1 - core]
        remote(spot, spot, done, sr.at[p], sib).wait_recv()

    def gather_drain(p):
        spot = gaths[p].at[core]
        remote(spot, spot, done, sr.at[p], sib).wait_send()
        part = gaths[p].at[core, pl.ds(0, depth - 1)]
        remote(part, part, done, zr.at[p, z], sib).wait_send()
        if cols > 1:
            part = gaths[p].at[core, pl.ds(0, depth)]
            remote(part, part, done, yr.at[p, z], y_peer).wait_send()

    def fill_pool(p):
        g = p // 2
        pool[p, :own_rows, :] = own[p].reshape(own_rows, dh)
        for s in range(n_far):
            owner = jnp.clip(tab[g, n + s, 0], 0, n - 1)
            block = jnp.clip(tab[g, n + s, 1], 0, own_blocks - 1)
            lo = own_rows + s * BLK
            pool[p, lo : lo + BLK, :] = gaths[p][owner & 1, owner >> 1, block]

    mates = [(y, 1 - core)] + ([(other_y, core), (other_y, 1 - core)] if cols > 1 else [])

    def mate_copy(p, m, zz):
        return remote(
            box.at[p, zz, m], box_in.at[p, zz, m], done, box_recv.at[p, zz],
            device(z, *mates[m]),
        )

    def z_copy(p, to_z):
        return remote(
            z_box.at[p, to_z], z_in.at[p, z], done, rz_recv.at[p], device(to_z, y, core)
        )

    def factor(p):
        return scaling if p % 2 == 0 else 1.0

    def far_part(p, dest):
        return acc[p, own_blocks + jnp.clip(tab[p // 2, dest, 0], 0, n_far - 1)]

    def far_first(k):
        return jnp.where(k == depth, z, near(jnp.maximum(depth - k, 1)))

    def return_start(p):
        g = p // 2

        @pl.loop(1, depth + 1)
        def _(k):
            zz = far_first(k)
            for m, (yy, cc) in enumerate(mates):
                dest = device(zz, yy, cc)
                keep = tab[g, dest, 1].astype(jnp.float32) * factor(p)
                box[p, zz, m] = (far_part(p, dest) * keep).astype(jnp.bfloat16)
            for m in range(len(mates)):
                mate_copy(p, m, zz).start()

    def merged(p, zz):
        g = p // 2
        dest = device(zz, y, core)
        spot = box_in.at[p, zz]
        remote(spot, spot, done, box_recv.at[p, zz], sib).wait_recv()
        parts = [far_part(p, dest) * (tab[g, dest, 1].astype(jnp.float32) * factor(p))]
        tables = [tab] + [mate_tab.at[m] for m in range(len(mates))]
        for m in range(len(mates)):
            parts.append(box_in[p, zz, m].astype(jnp.float32))
        for b in range(own_blocks):
            total = None
            for table, part in zip(tables, parts):
                share = part * jnp.where(table[g, dest, 2] == b, 1.0, 0.0)
                total = share if total is None else total + share
            yield b, total

    def return_column(p, i):
        lo, hi = span(i)

        @pl.loop(lo, hi)
        def _(k):
            to_z = far_first(k)
            for b, part in merged(p, to_z):
                z_box[p, to_z, b] = part.astype(jnp.bfloat16)
            z_copy(p, to_z).start()

    def return_own(p):
        for b, part in merged(p, z):
            total_ref[p, b] = part + acc[p, b] * factor(p)

    def return_end(p):
        part = z_in.at[p, pl.ds(0, depth - 1)]
        remote(part, part, done, rz_recv.at[p], sib).wait_recv()

        @pl.loop(1, depth)
        def _(k):
            from_z = near(k)
            total_ref[p] += z_in[p, from_z].astype(jnp.float32)

        whole = total_ref[p].reshape(own_rows, dh)
        mix_ref[p % 2, pl.ds(p // 2, own_rows, stride=groups), :] = whole

    def return_drain(p):
        part = box.at[p]
        remote(part, part, done, box_recv.at[p, 0], sib).wait_send()
        part = z_box.at[p, pl.ds(0, depth - 1)]
        remote(part, part, done, rz_recv.at[p], sib).wait_send()

    barrier = pltpu.get_barrier_semaphore()

    def greet(peer):
        pl.semaphore_signal(
            barrier, inc=1, device_id={"ctx": peer}, device_id_type=pl.DeviceIdType.MESH
        )

    @pl.loop(1, depth)
    def _(k):
        greet(device(near(k), y, core))

    for yy, cc in mates:
        greet(device(z, yy, cc))
    kv_loads = [
        pltpu.make_async_copy(k_hbm, raw_ref.at[0], in_sem.at[0]),
        pltpu.make_async_copy(v_hbm, raw_ref.at[1], in_sem.at[1]),
    ]
    sel_load = pltpu.make_async_copy(sel_hbm, sel_ref, in_sem.at[2])
    rest = [
        pltpu.make_async_copy(q_hbm, q_ref, in_sem.at[3]),
        pltpu.make_async_copy(do_hbm, do_ref, in_sem.at[4]),
    ]
    for load in kv_loads + [sel_load] + rest:
        load.start()
    for kv in range(2):
        kv_loads[kv].wait()
        mix_ref[kv, : own_rows * groups] = raw_ref[kv].astype(jnp.float32)
        for g in range(groups):
            rows = mix_ref[kv, pl.ds(g, own_rows, stride=groups), :].astype(jnp.bfloat16)
            own[2 * g + kv] = rows.reshape(own_blocks, BLK, dh)
    pl.semaphore_wait(barrier, depth - 1 + len(mates))
    gather_start(0)
    sel_load.wait()
    for g in range(groups):
        fill_tables(g, n, me, n_far, own_blocks, sel_ref, picked_ref, tab_ref)
    to_scalars = pltpu.make_async_copy(tab_ref, tab, in_sem.at[2])
    to_scalars.start()
    to_mates = [
        remote(
            tab_ref, mate_tab_ref.at[m], done, tab_sem, device(z, yy, cc)
        )
        for m, (yy, cc) in enumerate(mates)
    ]
    for copy in to_mates:
        copy.start()
    gather_start(1)
    to_scalars.wait()
    for load in rest:
        load.wait()
    for g in range(groups):
        fill_own(
            g, per_group, chunk_tokens, picked_ref[g], q_ref, do_ref, own, bias_ref.at[g],
            own_score_ref.at[g], own_peak_ref.at[g], own_slope_ref.at[g],
        )
        if g == 0:
            for p in range(2, pieces):
                gather_start(p)

    def run(steps):
        for name, *args in steps:
            {
                "z": z_step, "y": y_step, "end": gather_end, "pool": fill_pool,
                "start": return_start, "column": return_column,
                "own": return_own, "done": return_end,
            }[name](*args)

    K0, V0, K1, V1 = range(4) if groups == 2 else (0, 1, None, None)

    def stage(body, plan):
        @pl.loop(0, chunks)
        def _(c):
            body(c)
            for i, steps in enumerate(plan):
                @pl.when(c == min(i, chunks - 1))
                def _():
                    run(steps)

    def heads(g):
        return slice(g * per_group, (g + 1) * per_group)

    def between(plan):
        return lambda t: run(plan[t] if t < len(plan) else [])

    def weigh_stage(g, plan):
        work = Weigh(
            heads(g), chunk_tokens, bias_ref.at[g], own_score_ref.at[g], own_peak_ref.at[g],
            q_ref, do_ref, pool.at[2 * g], s_ref, e_ref, acc.at[2 * g + 1],
        )
        pipelined([work.scores, work.exponents, work.products], chunks, between(plan))

    def slope_stage(g, plan):
        work = Slope(
            heads(g), chunk_tokens, own_slope_ref.at[g], q_ref, do_ref, pool.at[2 * g + 1], s_ref, e_ref,
            ds_ref.at[g], acc.at[2 * g],
        )
        pipelined([work.scores, work.products], chunks, between(plan))

    def query_stage(g, plan):
        keys_t = pool[2 * g].T
        stage(lambda c: query_grad(c, heads(g), chunk_tokens, keys_t, ds_ref.at[g], dq_ref), plan)

    run([("y", K0, 0), ("z", K0, 0), ("z", K0, 1), ("z", K0, 2), ("y", V0, 0)])
    remote(mate_tab_ref, mate_tab_ref, done, tab_sem, sib).wait_recv()
    back = pltpu.make_async_copy(mate_tab_ref, mate_tab, in_sem.at[3])
    back.start()
    run([("y", K1, 0), ("y", V1, 0), ("z", V0, 0), ("z", V0, 1), ("z", V0, 2), ("y", K0, 1),
         ("y", K0, 2), ("y", K0, 3), ("end", K0), ("pool", K0)])
    back.wait()
    weigh_stage(0, [
        [],
        [("z", K1, 0)],
        [],
        [("z", K1, 1)],
        [("z", K1, 2), ("y", V0, 1)],
        [("z", V1, 0), ("y", V0, 2)],
    ])
    run([("z", V1, 1), ("y", V0, 3), ("end", V0), ("pool", V0)])
    slope_stage(0, [
        [("z", V1, 2), ("y", K1, 1)],
        [("y", K1, 2)],
        [("start", V0), ("y", K1, 3)],
        [],
    ])
    run([("start", K0), ("y", V1, 1), ("end", K1), ("pool", K1)])
    weigh_stage(1, [
        [],
        [("y", V1, 2)],
        [],
        [("y", V1, 3)],
        [("column", V0, 0)],
        [("column", V0, 1)],
    ])
    run([("start", V1), ("end", V1), ("pool", V1)])
    slope_stage(1, [
        [("column", V0, 2)],
        [],
        [],
        [("column", K0, 0)],
        [("column", K0, 1)],
    ])
    run([("start", K1), ("column", K0, 2), ("own", V0), ("own", K0)])
    query_stage(0, [
        [("column", V1, 0)],
        [("column", V1, 1)],
        [("column", V1, 2)],
        [("done", V0)],
    ])
    query_stage(1, [
        [],
        [("own", V1), ("column", K1, 0), ("column", K1, 1), ("column", K1, 2)],
        [("own", K1)],
        [("done", K0), ("done", V1)],
    ])
    run([("done", K1)])
    remote(mate_tab_ref, mate_tab_ref, done, tab_sem, sib).wait_send()
    for p in range(pieces):
        gather_drain(p)
        return_drain(p)
    key_out[...] = mix_ref[0, : own_rows * groups].astype(jnp.bfloat16)
    value_out[...] = mix_ref[1, : own_rows * groups].astype(jnp.bfloat16)


def store_kernel(*refs):
    count = (len(refs) - 1) // 2
    sem = refs[-1]
    copies = [
        pltpu.make_async_copy(refs[i], refs[count + i], sem.at[i]) for i in range(count)
    ]
    for copy in copies:
        copy.start()
    for copy in copies:
        copy.wait()


def store(arrays):
    return pl.pallas_call(
        store_kernel,
        out_shape=tuple(jax.ShapeDtypeStruct(a.shape, a.dtype) for a in arrays),
        in_specs=[pl.BlockSpec(memory_space=pltpu.VMEM)] * len(arrays),
        out_specs=(pl.BlockSpec(memory_space=pl.ANY),) * len(arrays),
        scratch_shapes=[pltpu.SemaphoreType.DMA((len(arrays),))],
    )(*arrays)


def columns_of(mesh, n):
    spots = [getattr(d, "coords", None) for d in mesh.devices.reshape(-1, n)[0]]
    if None in spots or n % 2:
        return 1
    cols = sum(spot[2] == spots[0][2] for spot in spots) // 2
    return 2 if cols == 2 and n % 4 == 0 else 1


def local(cols, queries, keys, values, grad_out, selected):
    tokens, head_count, dh = queries.shape
    groups = keys.shape[1]
    own_blocks = tokens // BLK
    n = lax.axis_size("ctx")
    depth = n // (2 * cols)
    chips = n // 2
    pieces = 2 * groups
    fetched = min(n - 2, max(selected.shape[2] - own_blocks, 4)) + 1
    slots = -(-(own_blocks + fetched) // 16) * 16
    far_rows = -(-fetched // 8) * 8
    pool_blocks = own_blocks + fetched
    pool_rows = pool_blocks * BLK
    chunk_tokens = min(tokens, 32)
    chunks = tokens // chunk_tokens
    rows = chunk_tokens * head_count // groups
    chosen = selected.transpose(1, 2, 0)
    mates = 3 if cols > 1 else 1
    any_spec = pl.BlockSpec(memory_space=pl.ANY)
    vmem = pl.BlockSpec(memory_space=pltpu.VMEM)
    dma = pltpu.SemaphoreType.DMA
    bf16, f32, i32 = jnp.bfloat16, jnp.float32, jnp.int32
    held = pl.pallas_call(
        functools.partial(fused_kernel, n, cols, fetched, chunk_tokens, groups),
        out_shape=(
            pltpu.VMEM(queries.shape, bf16),
            pltpu.VMEM((tokens * groups, dh), bf16),
            pltpu.VMEM((tokens * groups, dh), bf16),
        ),
        in_specs=[any_spec] * 5,
        out_specs=(vmem, vmem, vmem),
        scratch_shapes=[
            pltpu.VMEM(chosen.shape, i32),
            pltpu.VMEM(queries.shape, bf16),
            pltpu.VMEM(queries.shape, bf16),
            pltpu.VMEM((2, tokens * groups, dh), bf16),
            pltpu.VMEM((2, tokens * groups + 8, dh), f32),
            pltpu.VMEM((pieces, own_blocks, BLK, dh), bf16),
            pltpu.VMEM((pieces, pool_rows, dh), bf16),
            pltpu.VMEM((pieces, pool_blocks, BLK, dh), f32),
            pltpu.VMEM((2, pool_rows, rows), f32),
            pltpu.VMEM((chunks, pool_rows, rows), f32),
            pltpu.VMEM((groups, chunks, slots, rows), f32),
            pltpu.VMEM((groups, chunks, tokens, rows), f32),
            pltpu.VMEM((groups, chunks, 8, rows), f32),
            pltpu.VMEM((groups, chunks, tokens, rows), f32),
            pltpu.VMEM((groups, chunks, pool_rows, rows), bf16),
            pltpu.VMEM((groups, slots, tokens), bf16),
            pltpu.VMEM((groups, n + far_rows, LANES), i32),
            pltpu.VMEM((mates, groups, n + far_rows, LANES), i32),
            pltpu.SMEM((groups, n + far_rows, LANES), i32),
            pltpu.SMEM((mates, groups, n + far_rows, LANES), i32),
            pltpu.VMEM((pieces, depth, mates, BLK, dh), bf16),
            pltpu.VMEM((pieces, depth, mates, BLK, dh), bf16),
            pltpu.VMEM((pieces, depth, own_blocks, BLK, dh), bf16),
            pltpu.VMEM((pieces, depth, own_blocks, BLK, dh), bf16),
            pltpu.VMEM((pieces, own_blocks, BLK, dh), f32),
            dma((5,)),
            dma,
            dma,
            dma((pieces, depth)),
            dma((pieces, depth)),
            dma((pieces,)),
            dma((pieces, depth)),
            dma((pieces,)),
        ] + [pltpu.VMEM((2, chips, own_blocks, BLK, dh), bf16)] * pieces,
        compiler_params=pltpu.CompilerParams(collective_id=0, has_side_effects=True),
    )(
        chosen,
        queries,
        grad_out,
        keys.reshape(tokens * groups, dh),
        values.reshape(tokens * groups, dh),
    )
    held = [pltpu.with_memory_space_constraint(a, pltpu.VMEM) for a in held]
    dq, key_grad, value_grad = store(held)
    return dq, key_grad.reshape(keys.shape), value_grad.reshape(values.shape)


def solution(mesh):
    spec = P(("rep", "ctx"), None, None)
    cols = columns_of(mesh, mesh.shape["ctx"])
    return jax.shard_map(
        functools.partial(local, cols),
        mesh=mesh,
        in_specs=(spec,) * 5,
        out_specs=(spec,) * 3,
        check_vma=False,
    )
```
